32 devices in a mesh: data: 1 (over z), col: 4 (over y), row: 8 (over x, core).
Axes of the slice: x: 4, y: 4, z: 1, core: 2. Of those that a mesh axis runs over, the one named last changes fastest.
The devices are a block of a 4x4x8 slice.
Arguments:
- pair_rep: bfloat16 [768, 768, 128], P(('data', 'row'), 'col')
- res_mask: int32 [768], P('data')
- ln_gamma: float32 [128], replicated
- ln_beta: float32 [128], replicated
- w_q: bfloat16 [128, 128], replicated
- w_k: bfloat16 [128, 128], replicated
- w_v: bfloat16 [128, 128], replicated
- w_b: bfloat16 [128, 4], replicated
- w_g: bfloat16 [128, 128], replicated
- w_o: bfloat16 [128, 128], replicated
Outputs:
- output: bfloat16 [768, 768, 128], P(('data', 'row'), 'col')
All inputs are finite; a program needn't handle non-finite values.
Results may differ from the reference program's by a relative error of at most 0.00640002.
Values are sent between devices in bfloat16 or wider.
A program may use at most 768 MiB of HBM per device.

```python
import math
import jax
import jax.numpy as jnp
from jax import lax

N = 768
C_Z = 128
HEADS = 4
HEAD = 32

PROJ = HEADS * HEAD
Q_SCALE = 1.0 / math.sqrt(HEAD)
LN_EPS = 1e-5
MASK_FILL = -1e9
OUT_GAIN = 0.35 * math.sqrt(N / PROJ)


def setup_inputs(seed: int = 0, part: int = 0) -> dict:
    base_key = jax.random.key(seed)
    part_key = jax.random.fold_in(base_key, part)
    key_pair, key_len = jax.random.split(part_key, 2)
    pair_rep = jax.random.normal(key_pair, (N, N, C_Z), jnp.float32).astype(jnp.bfloat16)
    pad_len = jax.random.randint(key_len, (), N // 16, N // 4 + 1)
    res_mask = (jnp.arange(N) < N - pad_len).astype(jnp.int32)
    weight_keys = jax.random.split(base_key, 8)
    in_scale = 1.0 / math.sqrt(C_Z)
    ln_gamma = jax.random.uniform(weight_keys[0], (C_Z,), jnp.float32, 0.5, 1.5)
    ln_beta = 0.1 * jax.random.normal(weight_keys[1], (C_Z,), jnp.float32)
    w_q = (in_scale * jax.random.normal(weight_keys[2], (C_Z, PROJ), jnp.float32)).astype(jnp.bfloat16)
    w_k = (in_scale * jax.random.normal(weight_keys[3], (C_Z, PROJ), jnp.float32)).astype(jnp.bfloat16)
    w_v = (in_scale * jax.random.normal(weight_keys[4], (C_Z, PROJ), jnp.float32)).astype(jnp.bfloat16)
    w_b = (in_scale * jax.random.normal(weight_keys[5], (C_Z, HEADS), jnp.float32)).astype(jnp.bfloat16)
    w_g = (in_scale * jax.random.normal(weight_keys[6], (C_Z, PROJ), jnp.float32)).astype(jnp.bfloat16)
    w_o = (OUT_GAIN * jax.random.normal(weight_keys[7], (PROJ, C_Z), jnp.float32)).astype(jnp.bfloat16)
    return {'pair_rep': pair_rep, 'res_mask': res_mask, 'ln_gamma': ln_gamma, 'ln_beta': ln_beta, 'w_q': w_q, 'w_k': w_k, 'w_v': w_v, 'w_b': w_b, 'w_g': w_g, 'w_o': w_o}


def reference(pair_rep, res_mask, ln_gamma, ln_beta, w_q, w_k, w_v, w_b, w_g, w_o):
    pair_f32 = pair_rep.astype(jnp.float32)
    mean = jnp.mean(pair_f32, axis=-1, keepdims=True)
    centred = pair_f32 - mean
    variance = jnp.mean(centred * centred, axis=-1, keepdims=True)
    normed = (centred * lax.rsqrt(variance + LN_EPS) * ln_gamma + ln_beta).astype(jnp.bfloat16)
    bias = jnp.dot(normed.reshape(N * N, C_Z), w_b, preferred_element_type=jnp.float32).astype(jnp.bfloat16).reshape(N, N, HEADS)
    key_fill = jnp.where(res_mask > 0, 0.0, MASK_FILL).astype(jnp.float32)
    bias_ik = jnp.transpose(bias, (1, 0, 2)).astype(jnp.float32) + key_fill[None, :, None]

    def one_column(col_args):
        a_col, z_col = col_args
        query = (jnp.dot(a_col, w_q, preferred_element_type=jnp.float32) * Q_SCALE).astype(jnp.bfloat16).reshape(N, HEADS, HEAD)
        keys = jnp.dot(a_col, w_k, preferred_element_type=jnp.float32).astype(jnp.bfloat16).reshape(N, HEADS, HEAD)
        values = jnp.dot(a_col, w_v, preferred_element_type=jnp.float32).astype(jnp.bfloat16).reshape(N, HEADS, HEAD)
        gate = jax.nn.sigmoid(jnp.dot(a_col, w_g, preferred_element_type=jnp.float32))
        logits = jnp.einsum('ihd,khd->ikh', query.astype(jnp.float32), keys.astype(jnp.float32)) + bias_ik
        attn_prob = jax.nn.softmax(logits, axis=1)
        attended = jnp.einsum('ikh,khd->ihd', attn_prob, values.astype(jnp.float32)).reshape(N, PROJ)
        gated = (gate * attended).astype(jnp.bfloat16)
        return (z_col.astype(jnp.float32) + jnp.dot(gated, w_o, preferred_element_type=jnp.float32)).astype(jnp.bfloat16)

    out_cols = lax.map(one_column, (jnp.transpose(normed, (1, 0, 2)), jnp.transpose(pair_rep, (1, 0, 2))))
    return jnp.transpose(out_cols, (1, 0, 2))
```

```python
import functools
import math
import jax
import jax.numpy as jnp
from jax import lax
from jax.experimental import pallas as pl
from jax.experimental.pallas import tpu as pltpu
from jax.sharding import PartitionSpec as P

LN_EPS = 1e-5
MASK_FILL = -1e9
GROUP = 8
BLOCK = 256
F32 = jnp.float32
BF16 = jnp.bfloat16
NT = (((1,), (1,)), ((), ()))
TN = (((0,), (0,)), ((), ()))


def layer_norm(z, gamma, beta):
    mean = jnp.mean(z, axis=-1, keepdims=True)
    centred = z - mean
    variance = jnp.mean(centred * centred, axis=-1, keepdims=True)
    return centred * lax.rsqrt(variance + LN_EPS) * gamma + beta


def norm_group(z_ref, gamma, beta, a_scr, step=64):
    rows = z_ref.shape[0]

    def one(t, _):
        lo = pl.multiple_of(t * step, step)
        a = layer_norm(z_ref[pl.ds(lo, step)].astype(F32), gamma, beta)
        a_scr[pl.ds(pl.multiple_of(lo * GROUP, step * GROUP), step * GROUP), :] = a.reshape(step * GROUP, a.shape[-1])
        return 0

    lax.fori_loop(0, rows // step, one, 0)


def project_group(rows, a_scr, w_k, w_qvg_t, k_scr, q_scr, v_scr, g_scr, head_dim):
    proj = w_k.shape[1]

    def one(j, _):
        a = a_scr[pl.ds(j, rows, stride=GROUP), :].astype(BF16)
        k_scr[j] = jnp.dot(a, w_k[...], preferred_element_type=F32).astype(BF16)
        for lo in range(0, rows, BLOCK):
            t = lax.dot_general(w_qvg_t[...], a[lo:lo + BLOCK], NT, preferred_element_type=F32)
            q_scr[j, :, lo:lo + BLOCK] = (t[:proj] * (1.0 / math.sqrt(head_dim))).astype(BF16)
            v_scr[j, :, lo:lo + BLOCK] = t[proj:2 * proj].astype(BF16)
            g_scr[j, :, lo:lo + BLOCK] = jax.nn.sigmoid(t[2 * proj:])
        return 0

    lax.fori_loop(0, GROUP, one, 0)


def attend(j, lo, rows, heads, head_dim, bias_scr, k_scr, q_scr, v_scr, g_scr, s_scr, w_o):
    proj = heads * head_dim
    q_all = q_scr[j, :, pl.ds(lo, BLOCK)]
    gated = []
    for h in range(heads):
        hs = slice(h * head_dim, (h + 1) * head_dim)
        parts = []
        if h:
            parts.append(jnp.zeros((h * head_dim, BLOCK), BF16))
        parts.append(q_all[hs])
        if h < heads - 1:
            parts.append(jnp.zeros((proj - (h + 1) * head_dim, BLOCK), BF16))
        q_pad = jnp.concatenate(parts, axis=0)
        top = None
        for kc in range(0, rows, BLOCK):
            s = jnp.dot(k_scr[j, kc:kc + BLOCK], q_pad, preferred_element_type=F32) + bias_scr[h, kc:kc + BLOCK, pl.ds(lo, BLOCK)]
            s_scr[h, kc:kc + BLOCK] = s
            part = jnp.max(s.reshape(BLOCK // 8, 8, BLOCK), axis=0)
            top = part if top is None else jnp.maximum(top, part)
        top = jnp.max(top, axis=0, keepdims=True)
        total = None
        acc = None
        for kc in range(0, rows, BLOCK):
            p = jnp.exp(s_scr[h, kc:kc + BLOCK] - top)
            part = jnp.sum(p.reshape(BLOCK // 8, 8, BLOCK), axis=0)
            total = part if total is None else total + part
            o = jnp.dot(v_scr[j, hs, kc:kc + BLOCK], p.astype(BF16), preferred_element_type=F32)
            acc = o if acc is None else acc + o
        total = jnp.sum(total, axis=0, keepdims=True)
        gated.append((g_scr[j, hs, pl.ds(lo, BLOCK)] * (acc / total)).astype(BF16))
    gated = jnp.concatenate(gated, axis=0)
    return lax.dot_general(gated, w_o[...], TN, preferred_element_type=F32)


def attn_kernel(heads, z_ref, bias_ref, fill_ref, gamma_ref, beta_ref, w_k, w_qvg_t, w_o, out_ref,
                a_scr, k_scr, q_scr, v_scr, g_scr, bias_scr, s_scr):
    rows = z_ref.shape[0]
    head_dim = w_k.shape[1] // heads

    @pl.when(pl.program_id(0) == 0)
    def _():
        def one(t, _):
            lo = pl.multiple_of(t * 32, 32)
            for h in range(heads):
                bias_scr[h, pl.ds(lo, 32), :] = bias_ref[h, pl.ds(lo, 32), :].astype(F32) + fill_ref[pl.ds(lo, 32), :]
            return 0
        lax.fori_loop(0, rows // 32, one, 0)

    norm_group(z_ref, gamma_ref[...], beta_ref[...], a_scr)
    project_group(rows, a_scr, w_k, w_qvg_t, k_scr, q_scr, v_scr, g_scr, head_dim)

    def unit(t, _):
        j = lax.rem(t, GROUP)
        lo = pl.multiple_of((t // GROUP) * BLOCK, BLOCK)
        upd = attend(j, lo, rows, heads, head_dim, bias_scr, k_scr, q_scr, v_scr, g_scr, s_scr, w_o)
        a_scr[pl.ds(lo * GROUP + j, BLOCK, stride=GROUP), :] = upd
        return 0

    lax.fori_loop(0, GROUP * (rows // BLOCK), unit, 0)

    def fin(t, _):
        lo = pl.multiple_of(t * 64, 64)
        upd = a_scr[pl.ds(pl.multiple_of(lo * GROUP, 64 * GROUP), 64 * GROUP), :].reshape(64, GROUP, a_scr.shape[1])
        out_ref[pl.ds(lo, 64)] = (z_ref[pl.ds(lo, 64)].astype(F32) + upd).astype(BF16)
        return 0

    lax.fori_loop(0, rows // 64, fin, 0)


def attention(z_t, bias, fill, gamma, beta, w_k, w_qvg_t, w_o):
    rows, cols, chan = z_t.shape
    heads = bias.shape[0]
    proj = w_k.shape[1]
    full = lambda *shape: pl.BlockSpec(shape, lambda g: (0,) * len(shape), pipeline_mode=pl.Buffered(1))
    blk = pl.BlockSpec((rows, GROUP, chan), lambda g: (0, g, 0))
    return pl.pallas_call(
        functools.partial(attn_kernel, heads),
        grid=(cols // GROUP,),
        out_shape=jax.ShapeDtypeStruct(z_t.shape, BF16),
        in_specs=[blk, full(heads, rows, rows), full(rows, 1), full(1, chan), full(1, chan), full(chan, proj),
                  full(3 * proj, chan), full(proj, chan)],
        out_specs=blk,
        scratch_shapes=[
            pltpu.VMEM((rows * GROUP, chan), F32),
            pltpu.VMEM((GROUP, rows, proj), BF16),
            pltpu.VMEM((GROUP, proj, rows), BF16),
            pltpu.VMEM((GROUP, proj, rows), BF16),
            pltpu.VMEM((GROUP, proj, rows), F32),
            pltpu.VMEM((heads, rows, rows), F32),
            pltpu.VMEM((heads, rows, BLOCK), F32),
        ],
        compiler_params=pltpu.CompilerParams(vmem_limit_bytes=58 * 1024 * 1024),
        name="attend",
    )(z_t, bias, fill, gamma, beta, w_k, w_qvg_t, w_o)


def solution(mesh):
    def body(pair_tile, res_mask, ln_gamma, ln_beta, w_q, w_k, w_v, w_b, w_g, w_o):
        block, cols, chan = pair_tile.shape
        z_t = lax.all_to_all(pair_tile, 'row', 1, 0, tiled=True)
        normed = layer_norm(pair_tile.astype(F32), ln_gamma, ln_beta).astype(BF16)
        bias = jnp.einsum('kic,ch->hki', normed, w_b, preferred_element_type=F32).astype(BF16)
        bias = lax.all_gather(bias, 'row', axis=1, tiled=True)
        bias = lax.all_gather(bias, 'col', axis=2, tiled=True)
        fill = jnp.where(res_mask > 0, 0.0, MASK_FILL).astype(F32)[:, None]
        w_qvg_t = jnp.concatenate([w_q.T, w_v.T, w_g.T], axis=0)
        out_t = attention(z_t, bias, fill, ln_gamma[None], ln_beta[None], w_k, w_qvg_t, w_o)
        return lax.all_to_all(out_t, 'row', 0, 1, tiled=True)

    tile_spec = P(('data', 'row'), 'col', None)
    return jax.shard_map(body, mesh=mesh, in_specs=(tile_spec, P('data'), P(), P(), P(), P(), P(), P(), P(), P()), out_specs=tile_spec, check_vma=False)
```

```python
import functools
import math
import jax
import jax.numpy as jnp
from jax import lax
from jax.experimental import pallas as pl
from jax.experimental.pallas import tpu as pltpu
from jax.sharding import PartitionSpec as P

LN_EPS = 1e-5
MASK_FILL = -1e9
GROUP = 8
BLOCK = 256
F32 = jnp.float32
BF16 = jnp.bfloat16
NT = (((1,), (1,)), ((), ()))
TN = (((0,), (0,)), ((), ()))


def layer_norm(z, gamma, beta):
    mean = jnp.mean(z, axis=-1, keepdims=True)
    centred = z - mean
    variance = jnp.mean(centred * centred, axis=-1, keepdims=True)
    return centred * lax.rsqrt(variance + LN_EPS) * gamma + beta


def norm_group(z_ref, gamma, beta, a_scr, step=64):
    rows = z_ref.shape[0]

    def one(t, _):
        lo = pl.multiple_of(t * step, step)
        a = layer_norm(z_ref[pl.ds(lo, step)].astype(F32), gamma, beta)
        a_scr[pl.ds(pl.multiple_of(lo * GROUP, step * GROUP), step * GROUP), :] = a.reshape(step * GROUP, a.shape[-1])
        return 0

    lax.fori_loop(0, rows // step, one, 0)


def project_group(rows, a_scr, w_k, w_qvg_t, k_scr, q_scr, v_scr, g_scr, head_dim):
    proj = w_k.shape[1]

    def one(j, _):
        a = a_scr[pl.ds(j, rows, stride=GROUP), :].astype(BF16)
        k_scr[j] = jnp.dot(a, w_k[...], preferred_element_type=F32).astype(BF16)
        for lo in range(0, rows, BLOCK):
            t = lax.dot_general(w_qvg_t[...], a[lo:lo + BLOCK], NT, preferred_element_type=F32)
            for h in range(proj // head_dim):
                hs = slice(h * head_dim, (h + 1) * head_dim)
                q_scr[j, h, hs, lo:lo + BLOCK] = (t[hs] * (1.0 / math.sqrt(head_dim))).astype(BF16)
                v_scr[j, h, :, lo:lo + BLOCK] = t[proj:2 * proj][hs].astype(BF16)
                g_scr[j, h, :, lo:lo + BLOCK] = jax.nn.sigmoid(t[2 * proj:][hs])
        return 0

    lax.fori_loop(0, GROUP, one, 0)


KC = 256
HB = 4


def score_chunk(j, h, lo, kc, bias_scr, k_scr, q_scr):
    q_pad = q_scr[j, h, :, pl.ds(lo, BLOCK)]
    return jnp.dot(k_scr[j, kc:kc + KC], q_pad, preferred_element_type=F32) + bias_scr[h, kc:kc + KC, pl.ds(lo, BLOCK)]


def fold8(x, op):
    return op(x.reshape(x.shape[0] // 8, 8, x.shape[1]), axis=0)


def scores(j, h, hb, lo, rows, bias_scr, k_scr, q_scr, s_scr, top_scr):
    top = None
    for kc in range(0, rows, KC):
        s = score_chunk(j, h, lo, kc, bias_scr, k_scr, q_scr)
        s_scr[hb, kc:kc + KC] = s
        part = fold8(s, jnp.max)
        top = part if top is None else jnp.maximum(top, part)
    top_scr[hb] = jnp.max(top, axis=0, keepdims=True)


def soft_and_next(cur, nxt, hb, rows, bias_scr, k_scr, q_scr, v_scr, g_scr, s_scr, top_scr, o_scr):
    j, h, lo = cur
    nj, nh, nlo = nxt
    top = top_scr[hb]
    total = acc = ntop = None
    for kc in range(0, rows, KC):
        p = jnp.exp(s_scr[hb, kc:kc + KC] - top)
        part = fold8(p, jnp.sum)
        total = part if total is None else total + part
        o = jnp.dot(v_scr[j, h, :, kc:kc + KC], p.astype(BF16), preferred_element_type=F32)
        acc = o if acc is None else acc + o
        s = score_chunk(nj, nh, nlo, kc, bias_scr, k_scr, q_scr)
        s_scr[hb, kc:kc + KC] = s
        part = fold8(s, jnp.max)
        ntop = part if ntop is None else jnp.maximum(ntop, part)
    top_scr[hb] = jnp.max(ntop, axis=0, keepdims=True)
    total = jnp.sum(total, axis=0, keepdims=True)
    o_scr[j, h, :, pl.ds(lo, BLOCK)] = (g_scr[j, h, :, pl.ds(lo, BLOCK)] * (acc / total)).astype(BF16)


def attend_all(units, rows, heads, bias_scr, k_scr, q_scr, v_scr, g_scr, s_scr, top_scr, o_scr):
    per = heads // HB

    def where(t, hb):
        u = t // per
        return lax.rem(u, GROUP), lax.rem(t, per) * HB + hb, pl.multiple_of((u // GROUP) * BLOCK, BLOCK)

    n = units * per
    for hb in range(HB):
        j, h, lo = where(0, hb)
        scores(j, h, hb, lo, rows, bias_scr, k_scr, q_scr, s_scr, top_scr)

    def one(t, _):
        nt = jnp.minimum(t + 1, n - 1)
        for hb in range(HB):
            soft_and_next(where(t, hb), where(nt, hb), hb, rows, bias_scr, k_scr, q_scr, v_scr, g_scr, s_scr, top_scr, o_scr)
        return 0

    lax.fori_loop(0, n, one, 0)


def attn_kernel(heads, z_ref, bias_ref, fill_ref, gamma_ref, beta_ref, w_k, w_qvg_t, w_o, out_ref,
                a_scr, k_scr, q_scr, v_scr, g_scr, bias_scr, s_scr, top_scr, o_scr):
    rows = z_ref.shape[0]
    head_dim = w_k.shape[1] // heads

    @pl.when(pl.program_id(0) == 0)
    def _():
        def one(t, _):
            lo = pl.multiple_of(t * 32, 32)
            for h in range(heads):
                bias_scr[h, pl.ds(lo, 32), :] = bias_ref[h, pl.ds(lo, 32), :].astype(F32) + fill_ref[pl.ds(lo, 32), :]
            return 0
        lax.fori_loop(0, rows // 32, one, 0)
        q_scr[...] = jnp.zeros_like(q_scr)

    norm_group(z_ref, gamma_ref[...], beta_ref[...], a_scr)
    project_group(rows, a_scr, w_k, w_qvg_t, k_scr, q_scr, v_scr, g_scr, head_dim)

    attend_all(GROUP * (rows // BLOCK), rows, heads, bias_scr, k_scr, q_scr, v_scr, g_scr, s_scr, top_scr, o_scr)

    def unit(j, _):
        for lo in range(0, rows, BLOCK):
            gated = o_scr[j, :, :, lo:lo + BLOCK].reshape(heads * head_dim, BLOCK)
            upd = lax.dot_general(gated, w_o[...], TN, preferred_element_type=F32)
            a_scr[pl.ds(lo * GROUP + j, BLOCK, stride=GROUP), :] = upd
        return 0

    lax.fori_loop(0, GROUP, unit, 0)

    def fin(t, _):
        lo = pl.multiple_of(t * 64, 64)
        upd = a_scr[pl.ds(pl.multiple_of(lo * GROUP, 64 * GROUP), 64 * GROUP), :].reshape(64, GROUP, a_scr.shape[1])
        out_ref[pl.ds(lo, 64)] = (z_ref[pl.ds(lo, 64)].astype(F32) + upd).astype(BF16)
        return 0

    lax.fori_loop(0, rows // 64, fin, 0)


def attention(z_t, bias, fill, gamma, beta, w_k, w_qvg_t, w_o):
    rows, cols, chan = z_t.shape
    heads = bias.shape[0]
    proj = w_k.shape[1]
    full = lambda *shape: pl.BlockSpec(shape, lambda g: (0,) * len(shape), pipeline_mode=pl.Buffered(1))
    blk = pl.BlockSpec((rows, GROUP, chan), lambda g: (0, g, 0))
    return pl.pallas_call(
        functools.partial(attn_kernel, heads),
        grid=(cols // GROUP,),
        out_shape=jax.ShapeDtypeStruct(z_t.shape, BF16),
        in_specs=[blk, full(heads, rows, rows), full(rows, 1), full(1, chan), full(1, chan), full(chan, proj),
                  full(3 * proj, chan), full(proj, chan)],
        out_specs=blk,
        scratch_shapes=[
            pltpu.VMEM((rows * GROUP, chan), F32),
            pltpu.VMEM((GROUP, rows, proj), BF16),
            pltpu.VMEM((GROUP, heads, proj, rows), BF16),
            pltpu.VMEM((GROUP, heads, proj // heads, rows), BF16),
            pltpu.VMEM((GROUP, heads, proj // heads, rows), F32),
            pltpu.VMEM((heads, rows, rows), F32),
            pltpu.VMEM((HB, rows, BLOCK), F32),
            pltpu.VMEM((HB, 1, BLOCK), F32),
            pltpu.VMEM((GROUP, heads, proj // heads, rows), BF16),
        ],
        compiler_params=pltpu.CompilerParams(vmem_limit_bytes=58 * 1024 * 1024),
        name="attend",
    )(z_t, bias, fill, gamma, beta, w_k, w_qvg_t, w_o)


def solution(mesh):
    def body(pair_tile, res_mask, ln_gamma, ln_beta, w_q, w_k, w_v, w_b, w_g, w_o):
        block, cols, chan = pair_tile.shape
        z_t = lax.all_to_all(pair_tile, 'row', 1, 0, tiled=True)
        normed = layer_norm(pair_tile.astype(F32), ln_gamma, ln_beta).astype(BF16)
        bias = jnp.einsum('kic,ch->hki', normed, w_b, preferred_element_type=F32).astype(BF16)
        bias = lax.all_gather(bias, 'row', axis=1, tiled=True)
        bias = lax.all_gather(bias, 'col', axis=2, tiled=True)
        fill = jnp.where(res_mask > 0, 0.0, MASK_FILL).astype(F32)[:, None]
        w_qvg_t = jnp.concatenate([w_q.T, w_v.T, w_g.T], axis=0)
        out_t = attention(z_t, bias, fill, ln_gamma[None], ln_beta[None], w_k, w_qvg_t, w_o)
        return lax.all_to_all(out_t, 'row', 0, 1, tiled=True)

    tile_spec = P(('data', 'row'), 'col', None)
    return jax.shard_map(body, mesh=mesh, in_specs=(tile_spec, P('data'), P(), P(), P(), P(), P(), P(), P(), P()), out_specs=tile_spec, check_vma=False)
```

```python
import functools
import math
import jax
import jax.numpy as jnp
from jax import lax
from jax.experimental import pallas as pl
from jax.experimental.pallas import tpu as pltpu
from jax.sharding import PartitionSpec as P

LN_EPS = 1e-5
MASK_FILL = -1e9
GROUP = 8
BLOCK = 256
PIECE = 32
KC = 256
LANES = 128
HALF = 64
F32 = jnp.float32
BF16 = jnp.bfloat16
NT = (((1,), (1,)), ((), ()))
TN = (((0,), (0,)), ((), ()))
MESH = pl.DeviceIdType.MESH


def layer_norm(z, gamma, beta):
    mean = jnp.mean(z, axis=-1, keepdims=True)
    centred = z - mean
    variance = jnp.mean(centred * centred, axis=-1, keepdims=True)
    return centred * lax.rsqrt(variance + LN_EPS) * gamma + beta


def norm_group(zin, c, gamma, beta, a_scr, step=64):
    rows = zin.shape[1]

    def one(t, _):
        lo = pl.multiple_of(t * step, step)
        a = layer_norm(zin[c, pl.ds(lo, step)].astype(F32), gamma, beta)
        a_scr[pl.ds(pl.multiple_of(lo * GROUP, step * GROUP), step * GROUP), :] = a.reshape(step * GROUP, a.shape[-1])
        return 0

    lax.fori_loop(0, rows // step, one, 0)


def project_group(rows, a_scr, w_k, w_qvg_t, k_scr, q_scr, v_scr, g_scr, head_dim):
    proj = w_k.shape[1]

    def one(j, _):
        a = a_scr[pl.ds(j, rows, stride=GROUP), :].astype(BF16)
        k_scr[j] = jnp.dot(a, w_k[...], preferred_element_type=F32).astype(BF16)
        for lo in range(0, rows, BLOCK):
            t = lax.dot_general(w_qvg_t[...], a[lo:lo + BLOCK], NT, preferred_element_type=F32)
            for h in range(proj // head_dim):
                hs = slice(h * head_dim, (h + 1) * head_dim)
                q_scr[j, h, hs, lo:lo + BLOCK] = (t[hs] * (1.0 / math.sqrt(head_dim))).astype(BF16)
                v_scr[j, h, :, lo:lo + BLOCK] = t[proj:2 * proj][hs].astype(BF16)
                g_scr[j, h, :, lo:lo + BLOCK] = jax.nn.sigmoid(t[2 * proj:][hs])
        return 0

    lax.fori_loop(0, GROUP, one, 0)


def score_chunk(j, h, lo, kc, bias_scr, k_scr, q_scr):
    q_pad = q_scr[j, h, :, pl.ds(lo, BLOCK)]
    return jnp.dot(k_scr[j, kc:kc + KC], q_pad, preferred_element_type=F32) + bias_scr[h, kc:kc + KC, pl.ds(lo, BLOCK)]


def fold8(x, op):
    return op(x.reshape(x.shape[0] // 8, 8, x.shape[1]), axis=0)


def scores(j, h, lo, rows, bias_scr, k_scr, q_scr, s_scr, top_scr):
    top = None
    for kc in range(0, rows, KC):
        s = score_chunk(j, h, lo, kc, bias_scr, k_scr, q_scr)
        s_scr[h, kc:kc + KC] = s
        part = fold8(s, jnp.max)
        top = part if top is None else jnp.maximum(top, part)
    top_scr[h] = jnp.max(top, axis=0, keepdims=True)


def soft_and_next(j, lo, nj, nlo, h, rows, bias_scr, k_scr, q_scr, v_scr, g_scr, s_scr, top_scr, o_scr):
    top = top_scr[h]
    total = acc = ntop = None
    for kc in range(0, rows, KC):
        p = jnp.exp(s_scr[h, kc:kc + KC] - top)
        part = fold8(p, jnp.sum)
        total = part if total is None else total + part
        o = jnp.dot(v_scr[j, h, :, kc:kc + KC], p.astype(BF16), preferred_element_type=F32)
        acc = o if acc is None else acc + o
        s = score_chunk(nj, h, nlo, kc, bias_scr, k_scr, q_scr)
        s_scr[h, kc:kc + KC] = s
        part = fold8(s, jnp.max)
        ntop = part if ntop is None else jnp.maximum(ntop, part)
    top_scr[h] = jnp.max(ntop, axis=0, keepdims=True)
    total = jnp.sum(total, axis=0, keepdims=True)
    o_scr[j, h, :, pl.ds(lo, BLOCK)] = (g_scr[j, h, :, pl.ds(lo, BLOCK)] * (acc / total)).astype(BF16)


def swap_half(x):
    return pltpu.roll(x, HALF, 1)


def lower_half(shape):
    return lax.broadcasted_iota(jnp.int32, shape, len(shape) - 1) < HALF


def kernel(n_row, n_col, heads, z_ref, fill_ref, gamma_ref, beta_ref, w_k, w_qvg_t, w_b_t, w_o, out_ref,
           zown, zin, brecv, b_scr, a_scr, k_scr, q_scr, v_scr, g_scr, bias_scr, s_scr, top_scr, o_scr,
           own_sem, zin_sem, zsend_sem, bx_sem, bxs_sem, by_sem, bys_sem, bd_sem, bds_sem, out_sem, osend_sem):
    block, cols, chan = z_ref.shape
    rows = block * n_row
    share = cols // n_row
    n_group = share // GROUP
    head_dim = w_k.shape[1] // heads
    n_chip = n_row // 2
    me = lax.axis_index('row')
    my_col = lax.axis_index('col')
    mate = me + 1 - 2 * lax.rem(me, 2)
    gamma, beta = gamma_ref[...], beta_ref[...]

    def row_at(s):
        return lax.rem(me + s, n_row)

    def col_at(s):
        return lax.rem(my_col + s, n_col)

    own = [pltpu.make_async_copy(z_ref.at[pl.ds(q * (block // 4), block // 4)], zown.at[pl.ds(q * (block // 4), block // 4)], own_sem.at[q]) for q in range(4)]
    for cp in own:
        cp.start()

    barrier = pltpu.get_barrier_semaphore()
    for s in range(1, n_row):
        pl.semaphore_signal(barrier, inc=1, device_id={'row': row_at(s)}, device_id_type=MESH)
    for s in range(1, n_col):
        pl.semaphore_signal(barrier, inc=1, device_id={'col': col_at(s)}, device_id_type=MESH)
    pl.semaphore_wait(barrier, n_row + n_col - 2)

    my_rows = pl.ds(pl.multiple_of(me * block, block), block)

    def send_group(c):
        for s in range(1, n_row):
            to = row_at(s)
            pltpu.make_async_remote_copy(
                src_ref=z_ref.at[:, pl.ds(pl.multiple_of(to * share + c * GROUP, GROUP), GROUP), :],
                dst_ref=zin.at[c, my_rows], send_sem=zsend_sem.at[s], recv_sem=zin_sem.at[c],
                device_id={'row': to}, device_id_type=MESH).start()
        pltpu.make_async_copy(z_ref.at[:, pl.ds(pl.multiple_of(me * share + c * GROUP, GROUP), GROUP), :],
                              zin.at[c, my_rows], zin_sem.at[c]).start()

    send_group(0)

    per = 4

    def own_bias(t, _):
        for u in range(per):
            k = t * per + u
            a = layer_norm(zown[k].astype(F32), gamma, beta).astype(BF16)
            for half, lo in enumerate((0, cols - LANES)):
                b_scr[pl.ds(half * 8 * block + k, 8, stride=block), :] = lax.dot_general(
                    w_b_t[...], a[lo:lo + LANES], NT, preferred_element_type=F32)
        return 0

    for q in range(4):
        own[q].wait()
        lax.fori_loop(q * (block // 4 // per), (q + 1) * (block // 4 // per), own_bias, 0)

    low = lower_half((block, LANES))
    def own_part(half, h):
        return b_scr[half * 8 * block + h * block:half * 8 * block + (h + 1) * block, :]

    for h in range(heads):
        brecv[my_col, me, h] = own_part(0, h).astype(BF16)
    for h in range(0, heads, 2):
        brecv[my_col, me, heads + h // 2] = jnp.where(low, swap_half(own_part(1, h)), own_part(1, h + 1)).astype(BF16)

    def tile(c, r):
        return brecv.at[c, r]

    def to_chip(d):
        to = row_at(2 * d)
        return pltpu.make_async_remote_copy(src_ref=tile(my_col, me), dst_ref=tile(my_col, me), send_sem=bxs_sem.at[d],
                                            recv_sem=bx_sem.at[d], device_id={'row': to}, device_id_type=MESH)

    def to_col(e, d):
        r = row_at(n_row - 2 * d)
        return pltpu.make_async_remote_copy(src_ref=tile(my_col, r), dst_ref=tile(my_col, r), send_sem=bys_sem.at[e, d],
                                            recv_sem=by_sem.at[e, d], device_id={'col': col_at(e)}, device_id_type=MESH)

    def to_mate(e, d):
        c, r = col_at(n_col - e), row_at(n_row - 2 * d)
        return pltpu.make_async_remote_copy(src_ref=tile(c, r), dst_ref=tile(c, r), send_sem=bds_sem.at[e, d],
                                            recv_sem=bd_sem.at[e, d], device_id={'row': mate}, device_id_type=MESH)

    def forward(d):
        for e in range(1, n_col):
            to_col(e, d).start()
        to_mate(0, d).start()

    for d in range(1, n_chip):
        to_chip(d).start()
    forward(0)
    for c in range(1, n_group):
        send_group(c)

    q_scr[...] = jnp.zeros_like(q_scr)

    def prepare(c):
        pltpu.make_async_copy(zin.at[c], zin.at[c], zin_sem.at[c]).wait()
        norm_group(zin, c, gamma, beta, a_scr)
        project_group(rows, a_scr, w_k, w_qvg_t, k_scr, q_scr, v_scr, g_scr, head_dim)

    prepare(0)
    for d in range(1, n_chip):
        to_chip(d).wait_recv()
        forward(d)
    for d in range(n_chip):
        for e in range(1, n_col):
            to_col(e, d).wait_recv()
            to_mate(e, d).start()
    for e in range(n_col):
        for d in range(n_chip):
            to_mate(e, d).wait_recv()

    def widen(r, _):
        at = pl.ds(pl.multiple_of(r * block, block), block)
        fill = jnp.broadcast_to(fill_ref[at, :], (block, LANES))
        for c in range(0, n_col, 2):
            for h in range(heads):
                a0, a1 = brecv[c, r, h].astype(F32), swap_half(brecv[c + 1, r, h].astype(F32))
                b0, b1 = brecv[c, r, heads + h // 2].astype(F32), brecv[c + 1, r, heads + h // 2].astype(F32)
                if h % 2:
                    b0 = swap_half(b0)
                else:
                    b1 = swap_half(b1)
                lo = c * cols
                bias_scr[h, at, lo:lo + LANES] = a0 + fill
                bias_scr[h, at, lo + LANES:lo + 2 * LANES] = jnp.where(low, b0, a1) + fill
                bias_scr[h, at, lo + 2 * LANES:lo + 3 * LANES] = jnp.where(low, a1, b1) + fill
        return 0

    lax.fori_loop(0, n_row, widen, 0)

    n_block = rows // BLOCK
    first = me // 2

    def where(u):
        return lax.rem(u, GROUP), pl.multiple_of(lax.rem(u // GROUP + first, n_block) * BLOCK, BLOCK)

    def group(c, _):
        for h in range(heads):
            j, lo = where(0)
            scores(j, h, lo, rows, bias_scr, k_scr, q_scr, s_scr, top_scr)

        def one_block(b, _):
            def one(u, _):
                j, lo = where(u)
                nj, nlo = where(jnp.minimum(u + 1, GROUP * n_block - 1))
                for h in range(heads):
                    soft_and_next(j, lo, nj, nlo, h, rows, bias_scr, k_scr, q_scr, v_scr, g_scr, s_scr, top_scr, o_scr)
                return 0

            lax.fori_loop(b * GROUP, (b + 1) * GROUP, one, 0)
            _, lo = where(b * GROUP)

            def update(j, _):
                gated = o_scr[j, :, :, pl.ds(lo, BLOCK)].reshape(heads * head_dim, BLOCK)
                a_scr[pl.ds(lo * GROUP + j, BLOCK, stride=GROUP), :] = lax.dot_general(gated, w_o[...], TN, preferred_element_type=F32)
                return 0

            lax.fori_loop(0, GROUP, update, 0)

            def finish(t, _):
                at = pl.multiple_of(lo + t * HALF, HALF)
                upd = a_scr[pl.ds(pl.multiple_of(at * GROUP, HALF * GROUP), HALF * GROUP), :].reshape(HALF, GROUP, chan)
                zin[c, pl.ds(at, HALF)] = (zin[c, pl.ds(at, HALF)].astype(F32) + upd).astype(BF16)
                return 0

            lax.fori_loop(0, BLOCK // HALF, finish, 0)

            def send(t, _):
                seg = lo // PIECE + t
                to = seg // (block // PIECE)
                off = lax.rem(seg, block // PIECE) * PIECE
                src = zin.at[c, pl.ds(pl.multiple_of(seg * PIECE, PIECE), PIECE)]
                dst = out_ref.at[pl.ds(pl.multiple_of(off, PIECE), PIECE), pl.ds(pl.multiple_of(me * share + c * GROUP, GROUP), GROUP), :]

                @pl.when(to == me)
                def _():
                    pltpu.make_async_copy(src, dst, out_sem).start()

                @pl.when(to != me)
                def _():
                    pltpu.make_async_remote_copy(src_ref=src, dst_ref=dst, send_sem=osend_sem, recv_sem=out_sem,
                                                 device_id={'row': to}, device_id_type=MESH).start()
                return 0

            lax.fori_loop(0, BLOCK // PIECE, send, 0)
            return 0

        lax.fori_loop(0, n_block, one_block, 0)

        @pl.when(c < n_group - 1)
        def _():
            prepare(c + 1)
        return 0

    lax.fori_loop(0, n_group, group, 0)

    for s in range(1, n_row):
        pltpu.make_async_copy(z_ref.at[:, 0:share, :], z_ref.at[:, 0:share, :], zsend_sem.at[s]).wait()
    for d in range(1, n_chip):
        to_chip(d).wait_send()
    for d in range(n_chip):
        for e in range(1, n_col):
            to_col(e, d).wait_send()
        for e in range(n_col):
            to_mate(e, d).wait_send()
    pltpu.make_async_copy(zin.at[:, 0:rows - block], zin.at[:, 0:rows - block], osend_sem).wait()
    pltpu.make_async_copy(z_ref, out_ref, out_sem).wait()


def run(n_row, n_col, z, fill, gamma, beta, w_k, w_qvg_t, w_b_t, w_o, heads):
    block, cols, chan = z.shape
    rows, share, proj = block * n_row, cols // n_row, w_k.shape[1]
    n_group, n_chip, head_dim = share // GROUP, n_row // 2, proj // heads
    vmem = pl.BlockSpec(memory_space=pltpu.VMEM)
    hbm = pl.BlockSpec(memory_space=pl.ANY)
    dma = pltpu.SemaphoreType.DMA
    return pl.pallas_call(
        functools.partial(kernel, n_row, n_col, heads),
        out_shape=jax.ShapeDtypeStruct(z.shape, BF16),
        in_specs=[hbm] + [vmem] * 7,
        out_specs=hbm,
        scratch_shapes=[
            pltpu.VMEM((block, cols, chan), BF16),
            pltpu.VMEM((n_group, rows, GROUP, chan), BF16),
            pltpu.VMEM((n_col, n_row, heads + heads // 2, block, LANES), BF16),
            pltpu.VMEM((2 * 8 * block, LANES), F32),
            pltpu.VMEM((rows * GROUP, chan), F32),
            pltpu.VMEM((GROUP, rows, proj), BF16),
            pltpu.VMEM((GROUP, heads, proj, rows), BF16),
            pltpu.VMEM((GROUP, heads, head_dim, rows), BF16),
            pltpu.VMEM((GROUP, heads, head_dim, rows), F32),
            pltpu.VMEM((heads, rows, rows), F32),
            pltpu.VMEM((heads, rows, BLOCK), F32),
            pltpu.VMEM((heads, 1, BLOCK), F32),
            pltpu.VMEM((GROUP, heads, head_dim, rows), BF16),
            dma((4,)), dma((n_group,)), dma((n_row,)), dma((n_chip,)), dma((n_chip,)), dma((n_col, n_chip)), dma((n_col, n_chip)),
            dma((n_col, n_chip)), dma((n_col, n_chip)), dma, dma,
        ],
        compiler_params=pltpu.CompilerParams(vmem_limit_bytes=62 * 1024 * 1024, collective_id=0, has_side_effects=True),
        name="triangle",
    )(z, fill, gamma, beta, w_k, w_qvg_t, w_b_t, w_o)


def solution(mesh):
    n_row, n_col = mesh.shape['row'], mesh.shape['col']

    def body(pair_tile, res_mask, ln_gamma, ln_beta, w_q, w_k, w_v, w_b, w_g, w_o):
        heads = w_b.shape[1]
        fill = jnp.where(res_mask > 0, 0.0, MASK_FILL).astype(F32)[:, None]
        w_qvg_t = jnp.concatenate([w_q.T, w_v.T, w_g.T], axis=0)
        w_b_t = jnp.pad(w_b.T, ((0, 8 - heads), (0, 0)))
        return run(n_row, n_col, pair_tile, fill, ln_gamma[None], ln_beta[None], w_k, w_qvg_t, w_b_t, w_o, heads)

    tile_spec = P(('data', 'row'), 'col', None)
    return jax.shard_map(body, mesh=mesh, in_specs=(tile_spec, P('data'), P(), P(), P(), P(), P(), P(), P(), P()), out_specs=tile_spec, check_vma=False)
```

```python
import functools
import math
import jax
import jax.numpy as jnp
from jax import lax
from jax.experimental import pallas as pl
from jax.experimental.pallas import tpu as pltpu
from jax.sharding import PartitionSpec as P

LN_EPS = 1e-5
MASK_FILL = -1e9
GROUP = 8
BLOCK = 256
PIECE = 32
KC = 256
LANES = 128
HALF = 64
F32 = jnp.float32
BF16 = jnp.bfloat16
NT = (((1,), (1,)), ((), ()))
TN = (((0,), (0,)), ((), ()))
MESH = pl.DeviceIdType.MESH


def layer_norm(z, gamma, beta):
    mean = jnp.mean(z, axis=-1, keepdims=True)
    centred = z - mean
    variance = jnp.mean(centred * centred, axis=-1, keepdims=True)
    return centred * lax.rsqrt(variance + LN_EPS) * gamma + beta


def norm_group(zin, c, gamma, beta, a_scr, step=64):
    rows = zin.shape[1]

    def one(t, _):
        lo = pl.multiple_of(t * step, step)
        a = layer_norm(zin[c, pl.ds(lo, step)].astype(F32), gamma, beta)
        a_scr[pl.ds(pl.multiple_of(lo * GROUP, step * GROUP), step * GROUP), :] = a.reshape(step * GROUP, a.shape[-1])
        return 0

    lax.fori_loop(0, rows // step, one, 0)


def project_group(rows, a_scr, w_k, w_qvg_t, k_scr, q_scr, v_scr, g_scr, head_dim):
    proj = w_k.shape[1]

    def one(j, _):
        a = a_scr[pl.ds(j, rows, stride=GROUP), :].astype(BF16)
        k_scr[j] = jnp.dot(a, w_k[...], preferred_element_type=F32).astype(BF16)
        for lo in range(0, rows, BLOCK):
            t = lax.dot_general(w_qvg_t[...], a[lo:lo + BLOCK], NT, preferred_element_type=F32)
            for h in range(proj // head_dim):
                hs = slice(h * head_dim, (h + 1) * head_dim)
                q_scr[j, h, hs, lo:lo + BLOCK] = (t[hs] * (1.0 / math.sqrt(head_dim))).astype(BF16)
                v_scr[j, h, :, lo:lo + BLOCK] = t[proj:2 * proj][hs].astype(BF16)
                g_scr[j, h, :, lo:lo + BLOCK] = jax.nn.sigmoid(t[2 * proj:][hs])
        return 0

    lax.fori_loop(0, GROUP, one, 0)


def score_chunk(j, h, lo, kc, bias_scr, k_scr, q_scr):
    q_pad = q_scr[j, h, :, pl.ds(lo, BLOCK)]
    return jnp.dot(k_scr[j, kc:kc + KC], q_pad, preferred_element_type=F32) + bias_scr[h, kc:kc + KC, pl.ds(lo, BLOCK)]


def fold8(x, op):
    return op(x.reshape(x.shape[0] // 8, 8, x.shape[1]), axis=0)


def scores(j, h, lo, rows, bias_scr, k_scr, q_scr, s_scr, top_scr):
    top = None
    for kc in range(0, rows, KC):
        s = score_chunk(j, h, lo, kc, bias_scr, k_scr, q_scr)
        s_scr[h, kc:kc + KC] = s
        part = fold8(s, jnp.max)
        top = part if top is None else jnp.maximum(top, part)
    top_scr[h] = jnp.max(top, axis=0, keepdims=True)


def soft_and_next(j, lo, nj, nlo, h, rows, bias_scr, k_scr, q_scr, v_scr, g_scr, s_scr, top_scr, o_scr):
    top = top_scr[h]
    total = acc = ntop = None
    for kc in range(0, rows, KC):
        p = jnp.exp(s_scr[h, kc:kc + KC] - top)
        part = fold8(p, jnp.sum)
        total = part if total is None else total + part
        o = jnp.dot(v_scr[j, h, :, kc:kc + KC], p.astype(BF16), preferred_element_type=F32)
        acc = o if acc is None else acc + o
        s = score_chunk(nj, h, nlo, kc, bias_scr, k_scr, q_scr)
        s_scr[h, kc:kc + KC] = s
        part = fold8(s, jnp.max)
        ntop = part if ntop is None else jnp.maximum(ntop, part)
    top_scr[h] = jnp.max(ntop, axis=0, keepdims=True)
    total = jnp.sum(total, axis=0, keepdims=True)
    o_scr[j, h, :, pl.ds(lo, BLOCK)] = (g_scr[j, h, :, pl.ds(lo, BLOCK)] * (acc / total)).astype(BF16)


def swap_half(x):
    return pltpu.roll(x, HALF, 1)


def lower_half(shape):
    return lax.broadcasted_iota(jnp.int32, shape, len(shape) - 1) < HALF


def kernel(n_row, n_col, heads, z_ref, mask_ref, gamma_ref, beta_ref, w_q, w_k, w_v, w_b, w_g, w_o, out_ref,
           w_qvg_t, w_b_t, fill_scr, zown, zin, brecv, b_scr, a_scr, k_scr, q_scr, v_scr, g_scr, bias_scr, s_scr, top_scr, o_scr,
           own_sem, zin_sem, zsend_sem, bx_sem, bxs_sem, by_sem, bys_sem, bd_sem, bds_sem, out_sem, osend_sem):
    block, cols, chan = z_ref.shape
    rows = block * n_row
    share = cols // n_row
    n_group = share // GROUP
    head_dim = w_k.shape[1] // heads
    n_chip = n_row // 2
    me = lax.axis_index('row')
    my_col = lax.axis_index('col')
    mate = me + 1 - 2 * lax.rem(me, 2)
    gamma, beta = gamma_ref[...], beta_ref[...]

    def row_at(s):
        return lax.rem(me + s, n_row)

    def col_at(s):
        return lax.rem(my_col + s, n_col)

    own = [pltpu.make_async_copy(z_ref.at[pl.ds(q * (block // 4), block // 4)], zown.at[pl.ds(q * (block // 4), block // 4)], own_sem.at[q]) for q in range(4)]
    for cp in own:
        cp.start()

    proj = heads * head_dim
    for n, w in enumerate((w_q, w_v, w_g)):
        w_qvg_t[n * proj:(n + 1) * proj] = w[...].astype(F32).T.astype(BF16)
    eye = (lax.broadcasted_iota(jnp.int32, (chan, chan), 0) == lax.broadcasted_iota(jnp.int32, (chan, chan), 1)).astype(BF16)
    w_b_t[...] = jnp.zeros_like(w_b_t)
    w_b_t[0:heads] = lax.dot_general(w_b[...], eye, TN, preferred_element_type=F32).astype(BF16)
    fill_row = jnp.where(mask_ref[...] > 0, 0.0, MASK_FILL).astype(F32)
    for lo in range(0, rows, LANES):
        fill_scr[lo:lo + LANES] = jnp.broadcast_to(fill_row[:, lo:lo + LANES], (LANES, LANES)).T
    q_scr[...] = jnp.zeros_like(q_scr)

    barrier = pltpu.get_barrier_semaphore()
    for s in range(1, n_row):
        pl.semaphore_signal(barrier, inc=1, device_id={'row': row_at(s)}, device_id_type=MESH)
    for s in range(1, n_col):
        pl.semaphore_signal(barrier, inc=1, device_id={'col': col_at(s)}, device_id_type=MESH)
    pl.semaphore_wait(barrier, n_row + n_col - 2)

    def send_group(c, lo=0, n=block):
        for s in range(1, n_row):
            to = row_at(s)
            pltpu.make_async_remote_copy(
                src_ref=z_ref.at[lo:lo + n, pl.ds(pl.multiple_of(to * share + c * GROUP, GROUP), GROUP), :],
                dst_ref=zin.at[c, pl.ds(pl.multiple_of(me * block + lo, 16), n)], send_sem=zsend_sem.at[s], recv_sem=zin_sem.at[c],
                device_id={'row': to}, device_id_type=MESH).start()
        pltpu.make_async_copy(z_ref.at[lo:lo + n, pl.ds(pl.multiple_of(me * share + c * GROUP, GROUP), GROUP), :],
                              zin.at[c, pl.ds(pl.multiple_of(me * block + lo, 16), n)], zin_sem.at[c]).start()

    send_group(0, 0, block // 2)

    per = 8

    def own_bias(t, _):
        for u in range(per):
            k = t * per + u
            a = layer_norm(zown[k].astype(F32), gamma, beta).astype(BF16)
            for half, lo in enumerate((0, cols - LANES)):
                b_scr[pl.ds(half * 8 * block + k, 8, stride=block), :] = lax.dot_general(
                    w_b_t[...], a[lo:lo + LANES], NT, preferred_element_type=F32)
        return 0

    for q in range(4):
        own[q].wait()
        lax.fori_loop(q * (block // 4 // per), (q + 1) * (block // 4 // per), own_bias, 0)

    low = lower_half((block, LANES))
    def own_part(half, h):
        return b_scr[half * 8 * block + h * block:half * 8 * block + (h + 1) * block, :]

    for h in range(heads):
        brecv[my_col, me, h] = own_part(0, h).astype(BF16)
    for h in range(0, heads, 2):
        brecv[my_col, me, heads + h // 2] = jnp.where(low, swap_half(own_part(1, h)), own_part(1, h + 1)).astype(BF16)

    def tile(c, r):
        return brecv.at[c, r]

    def to_chip(d):
        to = row_at(2 * d)
        return pltpu.make_async_remote_copy(src_ref=tile(my_col, me), dst_ref=tile(my_col, me), send_sem=bxs_sem.at[d],
                                            recv_sem=bx_sem.at[d], device_id={'row': to}, device_id_type=MESH)

    def line(d):
        return row_at(n_row - 2 * d)

    def to_col(e, d):
        t = tile(my_col, line(d))
        return pltpu.make_async_remote_copy(src_ref=t, dst_ref=t, send_sem=bys_sem.at[e, d], recv_sem=by_sem.at[e, d],
                                            device_id={'col': col_at(e)}, device_id_type=MESH)

    def relay(d):
        e = 1 if d < n_chip // 2 else n_col - 1
        t = tile(col_at(n_col - e), line(d))
        return pltpu.make_async_remote_copy(src_ref=t, dst_ref=t, send_sem=bys_sem.at[2, d], recv_sem=by_sem.at[2, d],
                                            device_id={'col': col_at(e)}, device_id_type=MESH)

    def to_mate(e, d):
        t = tile(col_at(n_col - e), line(d))
        return pltpu.make_async_remote_copy(src_ref=t, dst_ref=t, send_sem=bds_sem.at[e, d], recv_sem=bd_sem.at[e, d],
                                            device_id={'row': mate}, device_id_type=MESH)

    near = (1, n_col - 1)

    def forward(d):
        for e in near:
            to_col(e, d).start()
        to_mate(0, d).start()

    for d in range(1, n_chip):
        to_chip(d).start()
    forward(0)
    send_group(0, block // 2, block // 2)
    for c in range(1, n_group):
        send_group(c)

    def widen(col):
        def rows_of(r, _, c):
            at = pl.ds(pl.multiple_of(r * block, block), block)
            fill = fill_scr[at]
            lo = c * cols
            for h in range(heads):
                a, b = brecv[c, r, h].astype(F32), brecv[c, r, heads + h // 2].astype(F32)
                if c % 2 == 0:
                    bias_scr[h, at, lo:lo + LANES] = a + fill
                    b = (swap_half(b) if h % 2 else b) + fill
                    bias_scr[h, at, lo + LANES:lo + LANES + HALF] = b[:, 0:HALF]
                else:
                    a = swap_half(a)
                    b = b if h % 2 else swap_half(b)
                    bias_scr[h, at, lo:lo + HALF] = (a + fill)[:, HALF:LANES]
                    bias_scr[h, at, lo + HALF:lo + HALF + LANES] = jnp.where(low, a, b) + fill
            return 0

        for c in range(n_col):
            @pl.when(col == c)
            def _():
                lax.fori_loop(0, n_row, functools.partial(rows_of, c=c), 0)

    def prepare(c):
        pltpu.make_async_copy(zin.at[c], zin.at[c], zin_sem.at[c]).wait()
        norm_group(zin, c, gamma, beta, a_scr)
        project_group(rows, a_scr, w_k, w_qvg_t, k_scr, q_scr, v_scr, g_scr, head_dim)

    for d in range(1, n_chip):
        to_chip(d).wait_recv()
        forward(d)
    for d in range(n_chip):
        for e in near:
            to_col(e, d).wait_recv()
            to_mate(e, d).start()
        relay(d).start()
    prepare(0)
    for e in (0,) + near:
        for d in range(n_chip):
            to_mate(e, d).wait_recv()

    def widen_near(t, _):
        widen(lax.rem(my_col + t + t // 2, n_col))
        return 0

    lax.fori_loop(0, 3, widen_near, 0)

    def far_to_mate():
        for d in range(n_chip):
            relay(d).wait_recv()
            to_mate(2, d).start()

    def far_ready():
        for d in range(n_chip):
            to_mate(2, d).wait_recv()
        widen(col_at(2))

    n_block = rows // BLOCK

    def group(c, _):
        first = jnp.where(c == 0, (my_col + 1) // 2, me // 2)

        def where(u):
            return lax.rem(u, GROUP), pl.multiple_of(lax.rem(u // GROUP + first, n_block) * BLOCK, BLOCK)

        for h in range(heads):
            j, lo = where(0)
            scores(j, h, lo, rows, bias_scr, k_scr, q_scr, s_scr, top_scr)

        def one_block(b, _):
            def one(u, _):
                @pl.when((c == 0) & (u == GROUP // 2 - 1))
                def _():
                    far_to_mate()

                @pl.when((c == 0) & (u == GROUP - 2))
                def _():
                    far_ready()

                j, lo = where(u)
                nj, nlo = where(jnp.minimum(u + 1, GROUP * n_block - 1))
                for h in range(heads):
                    soft_and_next(j, lo, nj, nlo, h, rows, bias_scr, k_scr, q_scr, v_scr, g_scr, s_scr, top_scr, o_scr)
                return 0

            lax.fori_loop(b * GROUP, (b + 1) * GROUP, one, 0)
            _, lo = where(b * GROUP)

            def update(j, _):
                gated = o_scr[j, :, :, pl.ds(lo, BLOCK)].reshape(heads * head_dim, BLOCK)
                a_scr[pl.ds(lo * GROUP + j, BLOCK, stride=GROUP), :] = lax.dot_general(gated, w_o[...], TN, preferred_element_type=F32)
                return 0

            lax.fori_loop(0, GROUP, update, 0)

            def finish(t, _):
                at = pl.multiple_of(lo + t * HALF, HALF)
                upd = a_scr[pl.ds(pl.multiple_of(at * GROUP, HALF * GROUP), HALF * GROUP), :].reshape(HALF, GROUP, chan)
                zin[c, pl.ds(at, HALF)] = (zin[c, pl.ds(at, HALF)].astype(F32) + upd).astype(BF16)
                return 0

            lax.fori_loop(0, BLOCK // HALF, finish, 0)

            def send(t, _):
                seg = lo // PIECE + t
                to = seg // (block // PIECE)
                off = lax.rem(seg, block // PIECE) * PIECE
                src = zin.at[c, pl.ds(pl.multiple_of(seg * PIECE, PIECE), PIECE)]
                dst = out_ref.at[pl.ds(pl.multiple_of(off, PIECE), PIECE), pl.ds(pl.multiple_of(me * share + c * GROUP, GROUP), GROUP), :]

                @pl.when(to == me)
                def _():
                    pltpu.make_async_copy(src, dst, out_sem).start()

                @pl.when(to != me)
                def _():
                    pltpu.make_async_remote_copy(src_ref=src, dst_ref=dst, send_sem=osend_sem, recv_sem=out_sem,
                                                 device_id={'row': to}, device_id_type=MESH).start()
                return 0

            lax.fori_loop(0, BLOCK // PIECE, send, 0)
            return 0

        lax.fori_loop(0, n_block, one_block, 0)

        @pl.when(c < n_group - 1)
        def _():
            prepare(c + 1)
        return 0

    lax.fori_loop(0, n_group, group, 0)

    for s in range(1, n_row):
        pltpu.make_async_copy(z_ref.at[:, 0:share, :], z_ref.at[:, 0:share, :], zsend_sem.at[s]).wait()
    for d in range(1, n_chip):
        to_chip(d).wait_send()
    for d in range(n_chip):
        for e in near:
            to_col(e, d).wait_send()
        relay(d).wait_send()
        for e in range(n_col):
            to_mate(e, d).wait_send()
    pltpu.make_async_copy(zin.at[:, 0:rows - block], zin.at[:, 0:rows - block], osend_sem).wait()
    pltpu.make_async_copy(z_ref, out_ref, out_sem).wait()


def run(n_row, n_col, z, mask, gamma, beta, w_q, w_k, w_v, w_b, w_g, w_o):
    block, cols, chan = z.shape
    rows, share, proj = block * n_row, cols // n_row, w_k.shape[1]
    heads = w_b.shape[1]
    n_group, n_chip, head_dim = share // GROUP, n_row // 2, proj // heads
    vmem = pl.BlockSpec(memory_space=pltpu.VMEM)
    hbm = pl.BlockSpec(memory_space=pl.ANY)
    dma = pltpu.SemaphoreType.DMA
    return pl.pallas_call(
        functools.partial(kernel, n_row, n_col, heads),
        out_shape=jax.ShapeDtypeStruct(z.shape, BF16),
        in_specs=[hbm] + [vmem] * 9,
        out_specs=hbm,
        scratch_shapes=[
            pltpu.VMEM((3 * proj, chan), BF16),
            pltpu.VMEM((8, chan), BF16),
            pltpu.VMEM((rows, LANES), F32),
            pltpu.VMEM((block, cols, chan), BF16),
            pltpu.VMEM((n_group, rows, GROUP, chan), BF16),
            pltpu.VMEM((n_col, n_row, heads + heads // 2, block, LANES), BF16),
            pltpu.VMEM((2 * 8 * block, LANES), F32),
            pltpu.VMEM((rows * GROUP, chan), F32),
            pltpu.VMEM((GROUP, rows, proj), BF16),
            pltpu.VMEM((GROUP, heads, proj, rows), BF16),
            pltpu.VMEM((GROUP, heads, head_dim, rows), BF16),
            pltpu.VMEM((GROUP, heads, head_dim, rows), F32),
            pltpu.VMEM((heads, rows, rows), F32),
            pltpu.VMEM((heads, rows, BLOCK), F32),
            pltpu.VMEM((heads, 1, BLOCK), F32),
            pltpu.VMEM((GROUP, heads, head_dim, rows), BF16),
            dma((4,)), dma((n_group,)), dma((n_row,)), dma((n_chip,)), dma((n_chip,)), dma((n_col, n_chip)), dma((n_col, n_chip)),
            dma((n_col, n_chip)), dma((n_col, n_chip)), dma, dma,
        ],
        compiler_params=pltpu.CompilerParams(vmem_limit_bytes=62 * 1024 * 1024, collective_id=0, has_side_effects=True),
        name="triangle",
    )(z, mask, gamma, beta, w_q, w_k, w_v, w_b, w_g, w_o)


def solution(mesh):
    n_row, n_col = mesh.shape['row'], mesh.shape['col']

    def body(pair_tile, res_mask, ln_gamma, ln_beta, w_q, w_k, w_v, w_b, w_g, w_o):
        return run(n_row, n_col, pair_tile, res_mask[None], ln_gamma[None], ln_beta[None], w_q, w_k, w_v, w_b, w_g, w_o)

    tile_spec = P(('data', 'row'), 'col', None)
    return jax.shard_map(body, mesh=mesh, in_specs=(tile_spec, P('data'), P(), P(), P(), P(), P(), P(), P(), P()), out_specs=tile_spec, check_vma=False)
```

```python
import functools
import math
import jax
import jax.numpy as jnp
from jax import lax
from jax.experimental import pallas as pl
from jax.experimental.pallas import tpu as pltpu
from jax.sharding import PartitionSpec as P

LN_EPS = 1e-5
FILL_PARTS = (-998244352.0, -1753088.0, -2560.0)
assert sum(FILL_PARTS) == -1e9
GROUP = 8
BLOCK = 256
PIECE = 32
KC = 384
LANES = 128
HALF = 64
UNROLL = 2
F32 = jnp.float32
BF16 = jnp.bfloat16
NT = (((1,), (1,)), ((), ()))
TN = (((0,), (0,)), ((), ()))
MESH = pl.DeviceIdType.MESH


def layer_norm(z, gamma, beta):
    mean = jnp.mean(z, axis=-1, keepdims=True)
    centred = z - mean
    variance = jnp.mean(centred * centred, axis=-1, keepdims=True)
    return centred * lax.rsqrt(variance + LN_EPS) * gamma + beta


def norm_group(zin, c, gamma, beta, a_scr, step=64):
    rows = zin.shape[1]

    def one(t, _):
        lo = pl.multiple_of(t * step, step)
        a = layer_norm(zin[c, pl.ds(lo, step)].astype(F32), gamma, beta)
        a_scr[pl.ds(pl.multiple_of(lo * GROUP, step * GROUP), step * GROUP), :] = a.reshape(step * GROUP, a.shape[-1])
        return 0

    lax.fori_loop(0, rows // step, one, 0)


def project_group(rows, a_scr, w_kk, w_qvg_t, fill_scr, k_scr, q_scr, v_scr, g_scr, head_dim):
    proj = w_qvg_t.shape[0] // 3
    heads = proj // head_dim

    def one(pair, _):
        cols = []
        for side in range(2):
            j = 2 * pair + side
            a = a_scr[pl.ds(j, rows, stride=GROUP), :].astype(BF16)
            cols.append(a)
            for lo in range(0, rows, 2 * LANES):
                t = lax.dot_general(w_qvg_t[...], a[lo:lo + 2 * LANES], NT, preferred_element_type=F32)
                for h in range(heads):
                    hs = slice(h * head_dim, (h + 1) * head_dim)
                    q = (t[hs] * (1.0 / math.sqrt(head_dim))).astype(BF16)
                    here = slice(side * head_dim, (side + 1) * head_dim)
                    for n in range(2):
                        q_scr[pair, h, lo // LANES + n, here, side * LANES:(side + 1) * LANES] = q[:, n * LANES:(n + 1) * LANES]
                    v_scr[pair, h, here, lo:lo + 2 * LANES] = t[proj:2 * proj][hs].astype(BF16)
                    g_scr[j, h, :, lo:lo + 2 * LANES] = jax.nn.sigmoid(t[2 * proj:][hs])
        a = jnp.concatenate(cols, axis=1)
        for lo in range(0, rows, 2 * LANES):
            fill = fill_scr[lo:lo + 2 * LANES]
            for h in range(0, heads, 2):
                k = jnp.dot(a[lo:lo + 2 * LANES], w_kk[:, h * LANES:(h + 2) * LANES], preferred_element_type=F32).astype(BF16)
                k_scr[pair, h, lo:lo + 2 * LANES] = k[:, 0:LANES] + fill
                k_scr[pair, h + 1, lo:lo + 2 * LANES] = k[:, LANES:2 * LANES] + fill
        return 0

    lax.fori_loop(0, GROUP // 2, one, 0)


def right_side(pair, h, ib, q_scr, tail_scr):
    return jnp.concatenate([q_scr[pair, h, ib], tail_scr[...]], axis=0)


def score_chunk(pair, h, ib, kc, right, bias_scr, k_scr):
    left = jnp.concatenate([k_scr[pair, h, kc:kc + KC], bias_scr[h, ib, kc:kc + KC]], axis=1)
    return jnp.dot(left, right, preferred_element_type=F32)


def fold8(x, op):
    return op(x.reshape(x.shape[0] // 8, 8, x.shape[1]), axis=0)


def scores(pair, ib, h, rows, tail_scr, bias_scr, k_scr, q_scr, s_scr, top_scr):
    top = None
    right = right_side(pair, h, ib, q_scr, tail_scr)
    for kc in range(0, rows, KC):
        s = score_chunk(pair, h, ib, kc, right, bias_scr, k_scr)
        s_scr[h, kc:kc + KC] = s
        part = fold8(s, jnp.max)
        top = part if top is None else jnp.maximum(top, part)
    top_scr[h] = jnp.max(top, axis=0, keepdims=True)


def soft_and_next(pair, ib, npair, nib, h, rows, tail_scr, bias_scr, k_scr, q_scr, v_scr, g_scr, s_scr, top_scr, o_scr):
    head_dim = g_scr.shape[2]
    top = top_scr[h]
    total = acc = ntop = None
    right = right_side(npair, h, nib, q_scr, tail_scr)
    for kc in range(0, rows, KC):
        p = jnp.exp(s_scr[h, kc:kc + KC] - top)
        part = fold8(p, jnp.sum)
        total = part if total is None else total + part
        o = jnp.dot(v_scr[pair, h, :, kc:kc + KC], p.astype(BF16), preferred_element_type=F32)
        acc = o if acc is None else acc + o
        s = score_chunk(npair, h, nib, kc, right, bias_scr, k_scr)
        s_scr[h, kc:kc + KC] = s
        part = fold8(s, jnp.max)
        ntop = part if ntop is None else jnp.maximum(ntop, part)
    top_scr[h] = jnp.max(ntop, axis=0, keepdims=True)
    total = jnp.sum(total, axis=0, keepdims=True)
    at = pl.ds(pl.multiple_of(ib * LANES, LANES), LANES)
    for side in range(2):
        lanes = slice(side * LANES, (side + 1) * LANES)
        o = acc[side * head_dim:(side + 1) * head_dim, lanes] / total[:, lanes]
        o_scr[2 * pair + side, h, :, at] = (g_scr[2 * pair + side, h, :, at] * o).astype(BF16)


def swap_half(x):
    return pltpu.roll(x, HALF, 1)


def lower_half(shape):
    return lax.broadcasted_iota(jnp.int32, shape, len(shape) - 1) < HALF


def kernel(n_row, n_col, heads, z_ref, mask_ref, gamma_ref, beta_ref, w_q, w_k, w_v, w_b, w_g, w_o, out_ref,
           w_qvg_t, w_b_t, w_kk, tail_scr, fill_scr, zown, zin, brecv, b_scr, a_scr, k_scr, q_scr, v_scr, g_scr, bias_scr, s_scr, top_scr, o_scr,
           own_sem, zin_sem, zsend_sem, bx_sem, bxs_sem, by_sem, bys_sem, bd_sem, bds_sem, out_sem, osend_sem):
    block, cols, chan = z_ref.shape
    rows = block * n_row
    share = cols // n_row
    n_group = share // GROUP
    head_dim = w_k.shape[1] // heads
    n_chip = n_row // 2
    me = lax.axis_index('row')
    my_col = lax.axis_index('col')
    mate = me + 1 - 2 * lax.rem(me, 2)
    gamma, beta = gamma_ref[...], beta_ref[...]

    def row_at(s):
        return lax.rem(me + s, n_row)

    def col_at(s):
        return lax.rem(my_col + s, n_col)

    own = [pltpu.make_async_copy(z_ref.at[pl.ds(q * (block // 4), block // 4)], zown.at[pl.ds(q * (block // 4), block // 4)], own_sem.at[q]) for q in range(4)]
    for cp in own:
        cp.start()

    proj = heads * head_dim
    for n, w in enumerate((w_q, w_v, w_g)):
        w_qvg_t[n * proj:(n + 1) * proj] = w[...].astype(F32).T.astype(BF16)
    eye = (lax.broadcasted_iota(jnp.int32, (chan, chan), 0) == lax.broadcasted_iota(jnp.int32, (chan, chan), 1)).astype(BF16)
    w_b_t[...] = jnp.zeros_like(w_b_t)
    w_b_t[0:heads] = lax.dot_general(w_b[...], eye, TN, preferred_element_type=F32).astype(BF16)
    w_kk[...] = jnp.zeros_like(w_kk)
    for h in range(heads):
        wide = w_k[:, h * head_dim:(h + 1) * head_dim]
        w_kk[0:chan, h * LANES:h * LANES + head_dim] = wide
        w_kk[chan:2 * chan, h * LANES + head_dim:h * LANES + 2 * head_dim] = wide
    row = lax.broadcasted_iota(jnp.int32, (LANES - 2 * head_dim, 2 * LANES), 0)
    tail_scr[0:LANES - 2 * head_dim] = jnp.where(row < len(FILL_PARTS), 1.0, 0.0).astype(BF16)
    tail_scr[LANES - 2 * head_dim:] = jnp.concatenate([eye, eye], axis=1)
    lane = lax.broadcasted_iota(jnp.int32, (LANES, LANES), 1)
    part = jnp.zeros((LANES, LANES), F32)
    for n, f in enumerate(FILL_PARTS):
        part = jnp.where(lane == 2 * head_dim + n, f, part)
    keep = mask_ref[...].astype(F32)
    for lo in range(0, rows, LANES):
        masked = jnp.broadcast_to(keep[:, lo:lo + LANES], (LANES, LANES)).T
        fill_scr[lo:lo + LANES] = jnp.where(masked > 0.5, 0.0, part).astype(BF16)
    q_scr[...] = jnp.zeros_like(q_scr)

    barrier = pltpu.get_barrier_semaphore()
    for s in range(1, n_row):
        pl.semaphore_signal(barrier, inc=1, device_id={'row': row_at(s)}, device_id_type=MESH)
    for s in range(1, n_col):
        pl.semaphore_signal(barrier, inc=1, device_id={'col': col_at(s)}, device_id_type=MESH)
    pl.semaphore_wait(barrier, n_row + n_col - 2)

    def send_group(c, lo=0, n=block):
        for s in range(1, n_row):
            to = row_at(s)
            pltpu.make_async_remote_copy(
                src_ref=z_ref.at[lo:lo + n, pl.ds(pl.multiple_of(to * share + c * GROUP, GROUP), GROUP), :],
                dst_ref=zin.at[c, pl.ds(pl.multiple_of(me * block + lo, 16), n)], send_sem=zsend_sem.at[s], recv_sem=zin_sem.at[c],
                device_id={'row': to}, device_id_type=MESH).start()
        pltpu.make_async_copy(z_ref.at[lo:lo + n, pl.ds(pl.multiple_of(me * share + c * GROUP, GROUP), GROUP), :],
                              zin.at[c, pl.ds(pl.multiple_of(me * block + lo, 16), n)], zin_sem.at[c]).start()

    send_group(0, 0, block // 2)

    per = 8

    def own_bias(t, _):
        for u in range(per):
            k = t * per + u
            a = layer_norm(zown[k].astype(F32), gamma, beta).astype(BF16)
            for half, lo in enumerate((0, cols - LANES)):
                b_scr[pl.ds(half * 8 * block + k, 8, stride=block), :] = lax.dot_general(
                    w_b_t[...], a[lo:lo + LANES], NT, preferred_element_type=F32)
        return 0

    for q in range(4):
        own[q].wait()
        lax.fori_loop(q * (block // 4 // per), (q + 1) * (block // 4 // per), own_bias, 0)

    low = lower_half((block, LANES))
    def own_part(half, h):
        return b_scr[half * 8 * block + h * block:half * 8 * block + (h + 1) * block, :]

    for h in range(heads):
        brecv[my_col, me, h] = own_part(0, h).astype(BF16)
    for h in range(0, heads, 2):
        brecv[my_col, me, heads + h // 2] = jnp.where(low, swap_half(own_part(1, h)), own_part(1, h + 1)).astype(BF16)

    def tile(c, r):
        return brecv.at[c, r]

    def to_chip(d):
        to = row_at(2 * d)
        return pltpu.make_async_remote_copy(src_ref=tile(my_col, me), dst_ref=tile(my_col, me), send_sem=bxs_sem.at[d],
                                            recv_sem=bx_sem.at[d], device_id={'row': to}, device_id_type=MESH)

    def line(d):
        return row_at(n_row - 2 * d)

    def to_col(e, d):
        t = tile(my_col, line(d))
        return pltpu.make_async_remote_copy(src_ref=t, dst_ref=t, send_sem=bys_sem.at[e, d], recv_sem=by_sem.at[e, d],
                                            device_id={'col': col_at(e)}, device_id_type=MESH)

    def relay(d):
        e = 1 if d < n_chip // 2 else n_col - 1
        t = tile(col_at(n_col - e), line(d))
        return pltpu.make_async_remote_copy(src_ref=t, dst_ref=t, send_sem=bys_sem.at[2, d], recv_sem=by_sem.at[2, d],
                                            device_id={'col': col_at(e)}, device_id_type=MESH)

    def to_mate(e, d):
        t = tile(col_at(n_col - e), line(d))
        return pltpu.make_async_remote_copy(src_ref=t, dst_ref=t, send_sem=bds_sem.at[e, d], recv_sem=bd_sem.at[e, d],
                                            device_id={'row': mate}, device_id_type=MESH)

    near = (1, n_col - 1)

    def forward(d):
        for e in near:
            to_col(e, d).start()
        to_mate(0, d).start()

    for d in range(1, n_chip):
        to_chip(d).start()
    forward(0)
    send_group(0, block // 2, block // 2)
    for c in range(1, n_group):
        send_group(c)

    def widen(col):
        def rows_of(r, _, c):
            at = pl.ds(pl.multiple_of(r * block, block), block)
            first = c * cols // LANES
            for h in range(heads):
                if c % 2 == 0:
                    bias_scr[h, first, at] = brecv[c, r, h]
                    b = brecv[c, r, heads + h // 2]
                    if h % 2:
                        b = swap_half(b.astype(F32)).astype(BF16)
                    bias_scr[h, first + 1, at, 0:HALF] = b[:, 0:HALF]
                else:
                    a = swap_half(brecv[c, r, h].astype(F32))
                    b = brecv[c, r, heads + h // 2].astype(F32)
                    b = b if h % 2 else swap_half(b)
                    bias_scr[h, first, at, HALF:LANES] = a.astype(BF16)[:, HALF:LANES]
                    bias_scr[h, first + 1, at] = jnp.where(low, a, b).astype(BF16)
            return 0

        for c in range(n_col):
            @pl.when(col == c)
            def _():
                lax.fori_loop(0, n_row, functools.partial(rows_of, c=c), 0)

    def prepare(c):
        pltpu.make_async_copy(zin.at[c], zin.at[c], zin_sem.at[c]).wait()
        norm_group(zin, c, gamma, beta, a_scr)
        project_group(rows, a_scr, w_kk, w_qvg_t, fill_scr, k_scr, q_scr, v_scr, g_scr, head_dim)

    for d in range(1, n_chip):
        to_chip(d).wait_recv()
        forward(d)
    for d in range(n_chip):
        for e in near:
            to_col(e, d).wait_recv()
            to_mate(e, d).start()
        relay(d).start()
    prepare(0)
    for e in (0,) + near:
        for d in range(n_chip):
            to_mate(e, d).wait_recv()

    def widen_near(t, _):
        widen(lax.rem(my_col + t + t // 2, n_col))
        return 0

    lax.fori_loop(0, 3, widen_near, 0)

    def far_to_mate():
        for d in range(n_chip):
            relay(d).wait_recv()
            to_mate(2, d).start()

    def far_ready():
        for d in range(n_chip):
            to_mate(2, d).wait_recv()
        widen(col_at(2))

    n_block = rows // BLOCK

    def group(c, _):
        first = jnp.where(c == 0, (my_col + 1) // 2, me // 2)

        def block_lo(b):
            return pl.multiple_of(lax.rem(b + first, n_block) * BLOCK, BLOCK)

        def where(u):
            v = lax.rem(u, GROUP)
            return lax.rem(v, GROUP // 2), block_lo(u // GROUP) // LANES + v // (GROUP // 2)

        for h in range(heads):
            pair, ib = where(0)
            scores(pair, ib, h, rows, tail_scr, bias_scr, k_scr, q_scr, s_scr, top_scr)

        def one_block(b, _):
            def one(u, _):
                @pl.when((c == 0) & (u == (GROUP // 2 - 2) // UNROLL))
                def _():
                    far_to_mate()

                @pl.when((c == 0) & (u == (GROUP - 2) // UNROLL))
                def _():
                    far_ready()

                for v in range(UNROLL):
                    pair, ib = where(u * UNROLL + v)
                    npair, nib = where(jnp.minimum(u * UNROLL + v + 1, GROUP * n_block - 1))
                    for h in range(heads):
                        soft_and_next(pair, ib, npair, nib, h, rows, tail_scr, bias_scr, k_scr, q_scr, v_scr, g_scr, s_scr, top_scr, o_scr)
                return 0

            lax.fori_loop(b * (GROUP // UNROLL), (b + 1) * (GROUP // UNROLL), one, 0)
            lo = block_lo(b)

            def update(j, _):
                gated = o_scr[j, :, :, pl.ds(lo, BLOCK)].reshape(heads * head_dim, BLOCK)
                a_scr[pl.ds(lo * GROUP + j, BLOCK, stride=GROUP), :] = lax.dot_general(gated, w_o[...], TN, preferred_element_type=F32)
                return 0

            lax.fori_loop(0, GROUP, update, 0)

            def finish(t, _):
                at = pl.multiple_of(lo + t * HALF, HALF)
                upd = a_scr[pl.ds(pl.multiple_of(at * GROUP, HALF * GROUP), HALF * GROUP), :].reshape(HALF, GROUP, chan)
                zin[c, pl.ds(at, HALF)] = (zin[c, pl.ds(at, HALF)].astype(F32) + upd).astype(BF16)
                return 0

            lax.fori_loop(0, BLOCK // HALF, finish, 0)

            def send(t, _):
                seg = lo // PIECE + t
                to = seg // (block // PIECE)
                off = lax.rem(seg, block // PIECE) * PIECE
                src = zin.at[c, pl.ds(pl.multiple_of(seg * PIECE, PIECE), PIECE)]
                dst = out_ref.at[pl.ds(pl.multiple_of(off, PIECE), PIECE), pl.ds(pl.multiple_of(me * share + c * GROUP, GROUP), GROUP), :]

                @pl.when(to == me)
                def _():
                    pltpu.make_async_copy(src, dst, out_sem).start()

                @pl.when(to != me)
                def _():
                    pltpu.make_async_remote_copy(src_ref=src, dst_ref=dst, send_sem=osend_sem, recv_sem=out_sem,
                                                 device_id={'row': to}, device_id_type=MESH).start()
                return 0

            lax.fori_loop(0, BLOCK // PIECE, send, 0)
            return 0

        lax.fori_loop(0, n_block, one_block, 0)

        @pl.when(c < n_group - 1)
        def _():
            prepare(c + 1)
        return 0

    lax.fori_loop(0, n_group, group, 0)

    for s in range(1, n_row):
        pltpu.make_async_copy(z_ref.at[:, 0:share, :], z_ref.at[:, 0:share, :], zsend_sem.at[s]).wait()
    for d in range(1, n_chip):
        to_chip(d).wait_send()
    for d in range(n_chip):
        for e in near:
            to_col(e, d).wait_send()
        relay(d).wait_send()
        for e in range(n_col):
            to_mate(e, d).wait_send()
    pltpu.make_async_copy(zin.at[:, 0:rows - block], zin.at[:, 0:rows - block], osend_sem).wait()
    pltpu.make_async_copy(z_ref, out_ref, out_sem).wait()


def run(n_row, n_col, z, mask, gamma, beta, w_q, w_k, w_v, w_b, w_g, w_o):
    block, cols, chan = z.shape
    rows, share, proj = block * n_row, cols // n_row, w_k.shape[1]
    heads = w_b.shape[1]
    n_group, n_chip, head_dim = share // GROUP, n_row // 2, proj // heads
    vmem = pl.BlockSpec(memory_space=pltpu.VMEM)
    hbm = pl.BlockSpec(memory_space=pl.ANY)
    dma = pltpu.SemaphoreType.DMA
    return pl.pallas_call(
        functools.partial(kernel, n_row, n_col, heads),
        out_shape=jax.ShapeDtypeStruct(z.shape, BF16),
        in_specs=[hbm] + [vmem] * 9,
        out_specs=hbm,
        scratch_shapes=[
            pltpu.VMEM((3 * proj, chan), BF16),
            pltpu.VMEM((8, chan), BF16),
            pltpu.VMEM((2 * chan, heads * LANES), BF16),
            pltpu.VMEM((2 * LANES - 2 * head_dim, 2 * LANES), BF16),
            pltpu.VMEM((rows, LANES), BF16),
            pltpu.VMEM((block, cols, chan), BF16),
            pltpu.VMEM((n_group, rows, GROUP, chan), BF16),
            pltpu.VMEM((n_col, n_row, heads + heads // 2, block, LANES), BF16),
            pltpu.VMEM((2 * 8 * block, LANES), F32),
            pltpu.VMEM((rows * GROUP, chan), F32),
            pltpu.VMEM((GROUP // 2, heads, rows, LANES), BF16),
            pltpu.VMEM((GROUP // 2, heads, rows // LANES, 2 * head_dim, 2 * LANES), BF16),
            pltpu.VMEM((GROUP // 2, heads, 2 * head_dim, rows), BF16),
            pltpu.VMEM((GROUP, heads, head_dim, rows), F32),
            pltpu.VMEM((heads, rows // LANES, rows, LANES), BF16),
            pltpu.VMEM((heads, rows, BLOCK), F32),
            pltpu.VMEM((heads, 1, BLOCK), F32),
            pltpu.VMEM((GROUP, heads, head_dim, rows), BF16),
            dma((4,)), dma((n_group,)), dma((n_row,)), dma((n_chip,)), dma((n_chip,)), dma((n_col, n_chip)), dma((n_col, n_chip)),
            dma((n_col, n_chip)), dma((n_col, n_chip)), dma, dma,
        ],
        compiler_params=pltpu.CompilerParams(vmem_limit_bytes=62 * 1024 * 1024, collective_id=0, has_side_effects=True),
        name="triangle",
    )(z, mask, gamma, beta, w_q, w_k, w_v, w_b, w_g, w_o)


def solution(mesh):
    n_row, n_col = mesh.shape['row'], mesh.shape['col']

    def body(pair_tile, res_mask, ln_gamma, ln_beta, w_q, w_k, w_v, w_b, w_g, w_o):
        return run(n_row, n_col, pair_tile, res_mask[None], ln_gamma[None], ln_beta[None], w_q, w_k, w_v, w_b, w_g, w_o)

    tile_spec = P(('data', 'row'), 'col', None)
    return jax.shard_map(body, mesh=mesh, in_specs=(tile_spec, P('data'), P(), P(), P(), P(), P(), P(), P(), P()), out_specs=tile_spec, check_vma=False)
```

```python
import functools
import math
import jax
import jax.numpy as jnp
from jax import lax
from jax.experimental import pallas as pl
from jax.experimental.pallas import tpu as pltpu
from jax.sharding import PartitionSpec as P

LN_EPS = 1e-5
FILL_PARTS = (-998244352.0, -1753088.0, -2560.0)
assert sum(FILL_PARTS) == -1e9
GROUP = 8
BLOCK = 256
PIECE = 32
KC = 384
LANES = 128
HALF = 64
UNROLL = 2
F32 = jnp.float32
BF16 = jnp.bfloat16
NT = (((1,), (1,)), ((), ()))
TN = (((0,), (0,)), ((), ()))
MESH = pl.DeviceIdType.MESH


def layer_norm(z, gamma, beta):
    mean = jnp.mean(z, axis=-1, keepdims=True)
    centred = z - mean
    variance = jnp.mean(centred * centred, axis=-1, keepdims=True)
    return centred * lax.rsqrt(variance + LN_EPS) * gamma + beta


def norm_group(zin, c, gamma, beta, a_scr, step=64):
    rows = zin.shape[1]

    def one(t, _):
        lo = pl.multiple_of(t * step, step)
        a = layer_norm(zin[c, pl.ds(lo, step)].astype(F32), gamma, beta)
        a_scr[pl.ds(pl.multiple_of(lo * GROUP, step * GROUP), step * GROUP), :] = a.reshape(step * GROUP, a.shape[-1])
        return 0

    lax.fori_loop(0, rows // step, one, 0)


def project_group(rows, a_scr, w_kk, w_qvg_t, fill_scr, k_scr, q_scr, v_scr, g_scr, head_dim):
    proj = w_qvg_t.shape[0] // 3
    heads = proj // head_dim

    def one(pair, _):
        cols = []
        for side in range(2):
            j = 2 * pair + side
            a = a_scr[pl.ds(j, rows, stride=GROUP), :].astype(BF16)
            cols.append(a)
            for lo in range(0, rows, 2 * LANES):
                t = lax.dot_general(w_qvg_t[...], a[lo:lo + 2 * LANES], NT, preferred_element_type=F32)
                for h in range(heads):
                    hs = slice(h * head_dim, (h + 1) * head_dim)
                    q = (t[hs] * (1.0 / math.sqrt(head_dim))).astype(BF16)
                    here = slice(side * head_dim, (side + 1) * head_dim)
                    for n in range(2):
                        q_scr[pair, h, lo // LANES + n, here, side * LANES:(side + 1) * LANES] = q[:, n * LANES:(n + 1) * LANES]
                    v_scr[pair, h, here, lo:lo + 2 * LANES] = t[proj:2 * proj][hs].astype(BF16)
                    g_scr[j, h, :, lo:lo + 2 * LANES] = jax.nn.sigmoid(t[2 * proj:][hs])
        a = jnp.concatenate(cols, axis=1)
        for lo in range(0, rows, 2 * LANES):
            fill = fill_scr[lo:lo + 2 * LANES]
            for h in range(0, heads, 2):
                k = jnp.dot(a[lo:lo + 2 * LANES], w_kk[:, h * LANES:(h + 2) * LANES], preferred_element_type=F32).astype(BF16)
                k_scr[pair, h, lo:lo + 2 * LANES] = k[:, 0:LANES] + fill
                k_scr[pair, h + 1, lo:lo + 2 * LANES] = k[:, LANES:2 * LANES] + fill
        return 0

    lax.fori_loop(0, GROUP // 2, one, 0)


def right_side(pair, h, ib, q_scr, tail_scr):
    return jnp.concatenate([q_scr[pair, h, ib], tail_scr[...]], axis=0)


def score_chunk(pair, h, ib, kc, right, bias_scr, k_scr):
    left = jnp.concatenate([k_scr[pair, h, kc:kc + KC], bias_scr[h, ib, kc:kc + KC]], axis=1)
    return jnp.dot(left, right, preferred_element_type=F32)


def fold8(x, op):
    return op(x.reshape(x.shape[0] // 8, 8, x.shape[1]), axis=0)


def scores(pair, ib, h, rows, tail_scr, bias_scr, k_scr, q_scr, s_scr, top_scr):
    top = None
    right = right_side(pair, h, ib, q_scr, tail_scr)
    for kc in range(0, rows, KC):
        s = score_chunk(pair, h, ib, kc, right, bias_scr, k_scr)
        s_scr[h, kc:kc + KC] = s
        part = fold8(s, jnp.max)
        top = part if top is None else jnp.maximum(top, part)
    top_scr[h] = jnp.max(top, axis=0, keepdims=True)


def soft_and_next(pair, ib, npair, nib, h, rows, tail_scr, bias_scr, k_scr, q_scr, v_scr, g_scr, s_scr, top_scr, o_scr):
    head_dim = g_scr.shape[2]
    top = top_scr[h]
    total = acc = ntop = None
    right = right_side(npair, h, nib, q_scr, tail_scr)
    for kc in range(0, rows, KC):
        p = jnp.exp(s_scr[h, kc:kc + KC] - top)
        part = fold8(p, jnp.sum)
        total = part if total is None else total + part
        o = jnp.dot(v_scr[pair, h, :, kc:kc + KC], p.astype(BF16), preferred_element_type=F32)
        acc = o if acc is None else acc + o
        s = score_chunk(npair, h, nib, kc, right, bias_scr, k_scr)
        s_scr[h, kc:kc + KC] = s
        part = fold8(s, jnp.max)
        ntop = part if ntop is None else jnp.maximum(ntop, part)
    top_scr[h] = jnp.max(ntop, axis=0, keepdims=True)
    total = jnp.sum(total, axis=0, keepdims=True)
    at = pl.ds(pl.multiple_of(ib * LANES, LANES), LANES)
    for side in range(2):
        lanes = slice(side * LANES, (side + 1) * LANES)
        o = acc[side * head_dim:(side + 1) * head_dim, lanes] / total[:, lanes]
        o_scr[2 * pair + side, h, :, at] = (g_scr[2 * pair + side, h, :, at] * o).astype(BF16)


def swap_half(x):
    return pltpu.roll(x, HALF, 1)


def lower_half(shape):
    return lax.broadcasted_iota(jnp.int32, shape, len(shape) - 1) < HALF


def kernel(n_row, n_col, heads, z_ref, mask_ref, gamma_ref, beta_ref, w_q, w_k, w_v, w_b, w_g, w_o, out_ref,
           w_qvg_t, w_b_t, w_kk, tail_scr, fill_scr, zown, zin, brecv, b_scr, a_scr, k_scr, q_scr, v_scr, g_scr, bias_scr, s_scr, top_scr, o_scr,
           own_sem, zin_sem, zsend_sem, bx_sem, bxs_sem, by_sem, bys_sem, bd_sem, bds_sem, out_sem, osend_sem):
    block, cols, chan = z_ref.shape
    rows = block * n_row
    share = cols // n_row
    n_group = share // GROUP
    head_dim = w_k.shape[1] // heads
    n_chip = n_row // 2
    me = lax.axis_index('row')
    my_col = lax.axis_index('col')
    mate = me + 1 - 2 * lax.rem(me, 2)
    gamma, beta = gamma_ref[...], beta_ref[...]

    def row_at(s):
        return lax.rem(me + s, n_row)

    def col_at(s):
        return lax.rem(my_col + s, n_col)

    own = [pltpu.make_async_copy(z_ref.at[pl.ds(q * (block // 4), block // 4)], zown.at[pl.ds(q * (block // 4), block // 4)], own_sem.at[q]) for q in range(4)]
    for cp in own:
        cp.start()

    proj = heads * head_dim
    for n, w in enumerate((w_q, w_v, w_g)):
        w_qvg_t[n * proj:(n + 1) * proj] = w[...].astype(F32).T.astype(BF16)
    eye = (lax.broadcasted_iota(jnp.int32, (chan, chan), 0) == lax.broadcasted_iota(jnp.int32, (chan, chan), 1)).astype(BF16)
    w_b_t[...] = jnp.zeros_like(w_b_t)
    w_b_t[0:heads] = w_b[...]
    w_kk[...] = jnp.zeros_like(w_kk)
    for h in range(heads):
        wide = w_k[:, h * head_dim:(h + 1) * head_dim]
        w_kk[0:chan, h * LANES:h * LANES + head_dim] = wide
        w_kk[chan:2 * chan, h * LANES + head_dim:h * LANES + 2 * head_dim] = wide
    row = lax.broadcasted_iota(jnp.int32, (LANES - 2 * head_dim, 2 * LANES), 0)
    tail_scr[0:LANES - 2 * head_dim] = jnp.where(row < len(FILL_PARTS), 1.0, 0.0).astype(BF16)
    tail_scr[LANES - 2 * head_dim:] = jnp.concatenate([eye, eye], axis=1)
    lane = lax.broadcasted_iota(jnp.int32, (LANES, LANES), 1)
    part = jnp.zeros((LANES, LANES), F32)
    for n, f in enumerate(FILL_PARTS):
        part = jnp.where(lane == 2 * head_dim + n, f, part)
    keep = mask_ref[...].astype(F32)
    for n in range(rows // LANES):
        masked = jnp.broadcast_to(keep[n:n + 1], (LANES, LANES)).T
        fill_scr[n * LANES:(n + 1) * LANES] = jnp.where(masked > 0.5, 0.0, part).astype(BF16)
    q_scr[...] = jnp.zeros_like(q_scr)

    barrier = pltpu.get_barrier_semaphore()
    for s in range(1, n_row):
        pl.semaphore_signal(barrier, inc=1, device_id={'row': row_at(s)}, device_id_type=MESH)
    for s in range(1, n_col):
        pl.semaphore_signal(barrier, inc=1, device_id={'col': col_at(s)}, device_id_type=MESH)
    pl.semaphore_wait(barrier, n_row + n_col - 2)

    def send_group(c, lo=0, n=block):
        for s in range(1, n_row):
            to = row_at(s)
            pltpu.make_async_remote_copy(
                src_ref=z_ref.at[lo:lo + n, pl.ds(pl.multiple_of(to * share + c * GROUP, GROUP), GROUP), :],
                dst_ref=zin.at[c, pl.ds(pl.multiple_of(me * block + lo, 16), n)], send_sem=zsend_sem.at[s], recv_sem=zin_sem.at[c],
                device_id={'row': to}, device_id_type=MESH).start()
        pltpu.make_async_copy(z_ref.at[lo:lo + n, pl.ds(pl.multiple_of(me * share + c * GROUP, GROUP), GROUP), :],
                              zin.at[c, pl.ds(pl.multiple_of(me * block + lo, 16), n)], zin_sem.at[c]).start()

    send_group(0, 0, block // 2)

    per = 8

    def own_bias(t, _):
        for u in range(per):
            k = t * per + u
            a = layer_norm(zown[k].astype(F32), gamma, beta).astype(BF16)
            for half, lo in enumerate((0, cols - LANES)):
                b_scr[pl.ds(half * 8 * block + k, 8, stride=block), :] = lax.dot_general(
                    w_b_t[...], a[lo:lo + LANES], NT, preferred_element_type=F32)
        return 0

    for q in range(4):
        own[q].wait()
        lax.fori_loop(q * (block // 4 // per), (q + 1) * (block // 4 // per), own_bias, 0)

    low = lower_half((block, LANES))
    def own_part(half, h):
        return b_scr[half * 8 * block + h * block:half * 8 * block + (h + 1) * block, :]

    for h in range(heads):
        brecv[my_col, me, h] = own_part(0, h).astype(BF16)
    for h in range(0, heads, 2):
        brecv[my_col, me, heads + h // 2] = jnp.where(low, swap_half(own_part(1, h)), own_part(1, h + 1)).astype(BF16)

    def tile(c, r):
        return brecv.at[c, r]

    def to_chip(d):
        to = row_at(2 * d)
        return pltpu.make_async_remote_copy(src_ref=tile(my_col, me), dst_ref=tile(my_col, me), send_sem=bxs_sem.at[d],
                                            recv_sem=bx_sem.at[d], device_id={'row': to}, device_id_type=MESH)

    def line(d):
        return row_at(n_row - 2 * d)

    def to_col(e, d):
        t = tile(my_col, line(d))
        return pltpu.make_async_remote_copy(src_ref=t, dst_ref=t, send_sem=bys_sem.at[e, d], recv_sem=by_sem.at[e, d],
                                            device_id={'col': col_at(e)}, device_id_type=MESH)

    def relay(d):
        e = 1 if d < n_chip // 2 else n_col - 1
        t = tile(col_at(n_col - e), line(d))
        return pltpu.make_async_remote_copy(src_ref=t, dst_ref=t, send_sem=bys_sem.at[2, d], recv_sem=by_sem.at[2, d],
                                            device_id={'col': col_at(e)}, device_id_type=MESH)

    def to_mate(e, d):
        t = tile(col_at(n_col - e), line(d))
        return pltpu.make_async_remote_copy(src_ref=t, dst_ref=t, send_sem=bds_sem.at[e, d], recv_sem=bd_sem.at[e, d],
                                            device_id={'row': mate}, device_id_type=MESH)

    near = (1, n_col - 1)

    def forward(d):
        for e in near:
            to_col(e, d).start()
        to_mate(0, d).start()

    for d in range(1, n_chip):
        to_chip(d).start()
    forward(0)

    def widen(col):
        def rows_of(r, _, c):
            at = pl.ds(pl.multiple_of(r * block, block), block)
            first = c * cols // LANES
            for h in range(heads):
                if c % 2 == 0:
                    bias_scr[h, first, at] = brecv[c, r, h]
                    b = brecv[c, r, heads + h // 2]
                    if h % 2:
                        b = swap_half(b.astype(F32)).astype(BF16)
                    bias_scr[h, first + 1, at, 0:HALF] = b[:, 0:HALF]
                else:
                    a = swap_half(brecv[c, r, h].astype(F32))
                    b = brecv[c, r, heads + h // 2].astype(F32)
                    b = b if h % 2 else swap_half(b)
                    bias_scr[h, first, at, HALF:LANES] = a.astype(BF16)[:, HALF:LANES]
                    bias_scr[h, first + 1, at] = jnp.where(low, a, b).astype(BF16)
            return 0

        for c in range(n_col):
            @pl.when(col == c)
            def _():
                lax.fori_loop(0, n_row, functools.partial(rows_of, c=c), 0)

    def arrived(c):
        pltpu.make_async_copy(zin.at[c], zin.at[c], zin_sem.at[c]).wait()

    def prepare(c):
        norm_group(zin, c, gamma, beta, a_scr)
        project_group(rows, a_scr, w_kk, w_qvg_t, fill_scr, k_scr, q_scr, v_scr, g_scr, head_dim)

    for d in range(1, n_chip):
        to_chip(d).wait_recv()
        forward(d)
    send_group(0, block // 2, block // 2)
    for d in range(n_chip):
        for e in near:
            to_col(e, d).wait_recv()
            to_mate(e, d).start()
        relay(d).start()
    arrived(0)
    send_group(1)
    prepare(0)
    for e in (0,) + near:
        for d in range(n_chip):
            to_mate(e, d).wait_recv()

    def widen_near(t, _):
        widen(lax.rem(my_col + t + t // 2, n_col))
        return 0

    lax.fori_loop(0, 3, widen_near, 0)

    def far_to_mate():
        for d in range(n_chip):
            relay(d).wait_recv()
            to_mate(2, d).start()

    def far_ready():
        for d in range(n_chip):
            to_mate(2, d).wait_recv()
        widen(col_at(2))

    n_block = rows // BLOCK

    def group(c, _):
        first = jnp.where(c == 0, (my_col + 1) // 2, me // 2)

        def block_lo(b):
            return pl.multiple_of(lax.rem(b + first, n_block) * BLOCK, BLOCK)

        def where(u):
            v = lax.rem(u, GROUP)
            return lax.rem(v, GROUP // 2), block_lo(u // GROUP) // LANES + v // (GROUP // 2)

        for h in range(heads):
            pair, ib = where(0)
            scores(pair, ib, h, rows, tail_scr, bias_scr, k_scr, q_scr, s_scr, top_scr)

        def one_block(b, _):
            def one(u, _):
                @pl.when((c == 0) & (u == (GROUP // 2 - 2) // UNROLL))
                def _():
                    far_to_mate()

                @pl.when((c == 0) & (u == (GROUP - 2) // UNROLL))
                def _():
                    far_ready()

                @pl.when((c == 0) & (u == (GROUP + GROUP // 2) // UNROLL))
                def _():
                    for g in range(2, n_group):
                        send_group(g)

                for v in range(UNROLL):
                    pair, ib = where(u * UNROLL + v)
                    npair, nib = where(jnp.minimum(u * UNROLL + v + 1, GROUP * n_block - 1))
                    for h in range(heads):
                        soft_and_next(pair, ib, npair, nib, h, rows, tail_scr, bias_scr, k_scr, q_scr, v_scr, g_scr, s_scr, top_scr, o_scr)
                return 0

            lax.fori_loop(b * (GROUP // UNROLL), (b + 1) * (GROUP // UNROLL), one, 0)
            lo = block_lo(b)

            def update(j, _):
                gated = o_scr[j, :, :, pl.ds(lo, BLOCK)].reshape(heads * head_dim, BLOCK)
                a_scr[pl.ds(lo * GROUP + j, BLOCK, stride=GROUP), :] = lax.dot_general(gated, w_o[...], TN, preferred_element_type=F32)
                return 0

            lax.fori_loop(0, GROUP, update, 0)

            def finish(t, _):
                at = pl.multiple_of(lo + t * HALF, HALF)
                upd = a_scr[pl.ds(pl.multiple_of(at * GROUP, HALF * GROUP), HALF * GROUP), :].reshape(HALF, GROUP, chan)
                zin[c, pl.ds(at, HALF)] = (zin[c, pl.ds(at, HALF)].astype(F32) + upd).astype(BF16)
                return 0

            lax.fori_loop(0, BLOCK // HALF, finish, 0)

            def send(t, _):
                seg = lo // PIECE + t
                to = seg // (block // PIECE)
                off = lax.rem(seg, block // PIECE) * PIECE
                src = zin.at[c, pl.ds(pl.multiple_of(seg * PIECE, PIECE), PIECE)]
                dst = out_ref.at[pl.ds(pl.multiple_of(off, PIECE), PIECE), pl.ds(pl.multiple_of(me * share + c * GROUP, GROUP), GROUP), :]

                @pl.when(to == me)
                def _():
                    pltpu.make_async_copy(src, dst, out_sem).start()

                @pl.when(to != me)
                def _():
                    pltpu.make_async_remote_copy(src_ref=src, dst_ref=dst, send_sem=osend_sem, recv_sem=out_sem,
                                                 device_id={'row': to}, device_id_type=MESH).start()
                return 0

            lax.fori_loop(0, BLOCK // PIECE, send, 0)
            return 0

        lax.fori_loop(0, n_block, one_block, 0)

        @pl.when(c < n_group - 1)
        def _():
            arrived(c + 1)
            prepare(c + 1)
        return 0

    lax.fori_loop(0, n_group, group, 0)

    for s in range(1, n_row):
        pltpu.make_async_copy(z_ref.at[:, 0:share, :], z_ref.at[:, 0:share, :], zsend_sem.at[s]).wait()
    for d in range(1, n_chip):
        to_chip(d).wait_send()
    for d in range(n_chip):
        for e in near:
            to_col(e, d).wait_send()
        relay(d).wait_send()
        for e in range(n_col):
            to_mate(e, d).wait_send()
    pltpu.make_async_copy(zin.at[:, 0:rows - block], zin.at[:, 0:rows - block], osend_sem).wait()
    pltpu.make_async_copy(z_ref, out_ref, out_sem).wait()


def run(n_row, n_col, z, mask, gamma, beta, w_q, w_k, w_v, w_b, w_g, w_o):
    block, cols, chan = z.shape
    rows, share, proj = block * n_row, cols // n_row, w_k.shape[1]
    heads = w_b.shape[0]
    n_group, n_chip, head_dim = share // GROUP, n_row // 2, proj // heads
    vmem = pl.BlockSpec(memory_space=pltpu.VMEM)
    hbm = pl.BlockSpec(memory_space=pl.ANY)
    dma = pltpu.SemaphoreType.DMA
    return pl.pallas_call(
        functools.partial(kernel, n_row, n_col, heads),
        out_shape=jax.ShapeDtypeStruct(z.shape, BF16),
        in_specs=[hbm] + [vmem] * 9,
        out_specs=hbm,
        scratch_shapes=[
            pltpu.VMEM((3 * proj, chan), BF16),
            pltpu.VMEM((8, chan), BF16),
            pltpu.VMEM((2 * chan, heads * LANES), BF16),
            pltpu.VMEM((2 * LANES - 2 * head_dim, 2 * LANES), BF16),
            pltpu.VMEM((rows, LANES), BF16),
            pltpu.VMEM((block, cols, chan), BF16),
            pltpu.VMEM((n_group, rows, GROUP, chan), BF16),
            pltpu.VMEM((n_col, n_row, heads + heads // 2, block, LANES), BF16),
            pltpu.VMEM((2 * 8 * block, LANES), F32),
            pltpu.VMEM((rows * GROUP, chan), F32),
            pltpu.VMEM((GROUP // 2, heads, rows, LANES), BF16),
            pltpu.VMEM((GROUP // 2, heads, rows // LANES, 2 * head_dim, 2 * LANES), BF16),
            pltpu.VMEM((GROUP // 2, heads, 2 * head_dim, rows), BF16),
            pltpu.VMEM((GROUP, heads, head_dim, rows), F32),
            pltpu.VMEM((heads, rows // LANES, rows, LANES), BF16),
            pltpu.VMEM((heads, rows, BLOCK), F32),
            pltpu.VMEM((heads, 1, BLOCK), F32),
            pltpu.VMEM((GROUP, heads, head_dim, rows), BF16),
            dma((4,)), dma((n_group,)), dma((n_row,)), dma((n_chip,)), dma((n_chip,)), dma((n_col, n_chip)), dma((n_col, n_chip)),
            dma((n_col, n_chip)), dma((n_col, n_chip)), dma, dma,
        ],
        compiler_params=pltpu.CompilerParams(vmem_limit_bytes=62 * 1024 * 1024, collective_id=0, has_side_effects=True),
        name="triangle",
    )(z, mask, gamma, beta, w_q, w_k, w_v, w_b, w_g, w_o)


def solution(mesh):
    n_row, n_col = mesh.shape['row'], mesh.shape['col']

    def body(pair_tile, res_mask, ln_gamma, ln_beta, w_q, w_k, w_v, w_b, w_g, w_o):
        return run(n_row, n_col, pair_tile, res_mask.reshape(-1, LANES), ln_gamma[None], ln_beta[None], w_q, w_k, w_v, w_b.T, w_g, w_o)

    tile_spec = P(('data', 'row'), 'col', None)
    return jax.shard_map(body, mesh=mesh, in_specs=(tile_spec, P('data'), P(), P(), P(), P(), P(), P(), P(), P()), out_specs=tile_spec, check_vma=False)
```

```python
import functools
import math
import jax
import jax.numpy as jnp
from jax import lax
from jax.experimental import pallas as pl
from jax.experimental.pallas import tpu as pltpu
from jax.sharding import PartitionSpec as P

LN_EPS = 1e-5
FILL_PARTS = (-998244352.0, -1753088.0, -2560.0)
assert sum(FILL_PARTS) == -1e9
GROUP = 8
BLOCK = 256
PIECE = 32
KC = 384
LANES = 128
HALF = 64
UNROLL = 2
F32 = jnp.float32
BF16 = jnp.bfloat16
NT = (((1,), (1,)), ((), ()))
TN = (((0,), (0,)), ((), ()))
MESH = pl.DeviceIdType.MESH


def layer_norm(z, gamma, beta):
    mean = jnp.mean(z, axis=-1, keepdims=True)
    centred = z - mean
    variance = jnp.mean(centred * centred, axis=-1, keepdims=True)
    return centred * lax.rsqrt(variance + LN_EPS) * gamma + beta


def norm_group(zin, c, gamma, beta, a_scr, step=64):
    rows = zin.shape[1]

    def one(t, _):
        lo = pl.multiple_of(t * step, step)
        a = layer_norm(zin[c, pl.ds(lo, step)].astype(F32), gamma, beta)
        a_scr[pl.ds(pl.multiple_of(lo * GROUP, step * GROUP), step * GROUP), :] = a.reshape(step * GROUP, a.shape[-1])
        return 0

    lax.fori_loop(0, rows // step, one, 0)


def project_group(rows, a_scr, w_kk, w_qvg_t, fill_scr, k_scr, q_scr, v_scr, g_scr, head_dim):
    proj = w_qvg_t.shape[0] // 3
    heads = proj // head_dim

    def one(pair, _):
        cols = []
        for side in range(2):
            j = 2 * pair + side
            a = a_scr[pl.ds(j, rows, stride=GROUP), :].astype(BF16)
            cols.append(a)
            for lo in range(0, rows, 2 * LANES):
                t = lax.dot_general(w_qvg_t[...], a[lo:lo + 2 * LANES], NT, preferred_element_type=F32)
                for h in range(heads):
                    hs = slice(h * head_dim, (h + 1) * head_dim)
                    q = (t[hs] * (1.0 / math.sqrt(head_dim))).astype(BF16)
                    here = slice(side * head_dim, (side + 1) * head_dim)
                    for n in range(2):
                        q_scr[pair, h, lo // LANES + n, here, side * LANES:(side + 1) * LANES] = q[:, n * LANES:(n + 1) * LANES]
                    v_scr[pair, h, here, lo:lo + 2 * LANES] = t[proj:2 * proj][hs].astype(BF16)
                    g_scr[j, h, :, lo:lo + 2 * LANES] = jax.nn.sigmoid(t[2 * proj:][hs])
        a = jnp.concatenate(cols, axis=1)
        for lo in range(0, rows, 2 * LANES):
            fill = fill_scr[lo:lo + 2 * LANES]
            for h in range(0, heads, 2):
                k = jnp.dot(a[lo:lo + 2 * LANES], w_kk[:, h * LANES:(h + 2) * LANES], preferred_element_type=F32).astype(BF16)
                k_scr[pair, h, lo:lo + 2 * LANES] = k[:, 0:LANES] + fill
                k_scr[pair, h + 1, lo:lo + 2 * LANES] = k[:, LANES:2 * LANES] + fill
        return 0

    lax.fori_loop(0, GROUP // 2, one, 0)


def right_side(pair, h, ib, q_scr, tail_scr):
    return jnp.concatenate([q_scr[pair, h, ib], tail_scr[...]], axis=0)


def score_chunk(pair, h, ib, kc, right, bias_scr, k_scr):
    left = jnp.concatenate([k_scr[pair, h, kc:kc + KC], bias_scr[h, ib, kc:kc + KC]], axis=1)
    return jnp.dot(left, right, preferred_element_type=F32)


def fold8(x, op):
    return op(x.reshape(x.shape[0] // 8, 8, x.shape[1]), axis=0)


def scores(pair, ib, h, rows, tail_scr, bias_scr, k_scr, q_scr, s_scr, top_scr):
    top = None
    right = right_side(pair, h, ib, q_scr, tail_scr)
    for kc in range(0, rows, KC):
        s = score_chunk(pair, h, ib, kc, right, bias_scr, k_scr)
        s_scr[h, kc:kc + KC] = s
        part = fold8(s, jnp.max)
        top = part if top is None else jnp.maximum(top, part)
    top_scr[h] = jnp.max(top, axis=0, keepdims=True)


def soft_and_next(pair, ib, npair, nib, h, rows, tail_scr, bias_scr, k_scr, q_scr, v_scr, g_scr, s_scr, top_scr, o_scr):
    head_dim = g_scr.shape[2]
    top = top_scr[h]
    total = acc = ntop = None
    right = right_side(npair, h, nib, q_scr, tail_scr)
    for kc in range(0, rows, KC):
        p = jnp.exp(s_scr[h, kc:kc + KC] - top)
        part = fold8(p, jnp.sum)
        total = part if total is None else total + part
        o = jnp.dot(v_scr[pair, h, :, kc:kc + KC], p.astype(BF16), preferred_element_type=F32)
        acc = o if acc is None else acc + o
        s = score_chunk(npair, h, nib, kc, right, bias_scr, k_scr)
        s_scr[h, kc:kc + KC] = s
        part = fold8(s, jnp.max)
        ntop = part if ntop is None else jnp.maximum(ntop, part)
    top_scr[h] = jnp.max(ntop, axis=0, keepdims=True)
    total = jnp.sum(total, axis=0, keepdims=True)
    at = pl.ds(pl.multiple_of(ib * LANES, LANES), LANES)
    for side in range(2):
        lanes = slice(side * LANES, (side + 1) * LANES)
        o = acc[side * head_dim:(side + 1) * head_dim, lanes] / total[:, lanes]
        o_scr[2 * pair + side, h, :, at] = (g_scr[2 * pair + side, h, :, at] * o).astype(BF16)


def swap_half(x):
    return pltpu.roll(x, HALF, 1)


def lower_half(shape):
    return lax.broadcasted_iota(jnp.int32, shape, len(shape) - 1) < HALF


def kernel(n_row, n_col, heads, z_ref, mask_ref, gamma_ref, beta_ref, w_q, w_k, w_v, w_b, w_g, w_o, out_ref,
           w_qvg_t, w_b_t, w_kk, tail_scr, fill_scr, zown, zin, brecv, b_scr, a_scr, k_scr, q_scr, v_scr, g_scr, bias_scr, s_scr, top_scr, o_scr,
           own_sem, zin_sem, zsend_sem, bx_sem, bxs_sem, by_sem, bys_sem, bd_sem, bds_sem, out_sem, osend_sem):
    block, cols, chan = z_ref.shape
    rows = block * n_row
    share = cols // n_row
    n_group = share // GROUP
    head_dim = w_k.shape[1] // heads
    n_chip = n_row // 2
    me = lax.axis_index('row')
    my_col = lax.axis_index('col')
    mate = me + 1 - 2 * lax.rem(me, 2)
    gamma, beta = gamma_ref[...], beta_ref[...]

    def row_at(s):
        return lax.rem(me + s, n_row)

    def col_at(s):
        return lax.rem(my_col + s, n_col)

    own = [pltpu.make_async_copy(z_ref.at[pl.ds(q * (block // 4), block // 4)], zown.at[pl.ds(q * (block // 4), block // 4)], own_sem.at[q]) for q in range(4)]
    for cp in own:
        cp.start()

    proj = heads * head_dim
    for n, w in enumerate((w_q, w_v, w_g)):
        w_qvg_t[n * proj:(n + 1) * proj] = w[...].astype(F32).T.astype(BF16)
    eye = (lax.broadcasted_iota(jnp.int32, (chan, chan), 0) == lax.broadcasted_iota(jnp.int32, (chan, chan), 1)).astype(BF16)
    w_b_t[...] = jnp.zeros_like(w_b_t)
    w_b_t[0:heads] = w_b[...]
    w_kk[...] = jnp.zeros_like(w_kk)
    for h in range(heads):
        wide = w_k[:, h * head_dim:(h + 1) * head_dim]
        w_kk[0:chan, h * LANES:h * LANES + head_dim] = wide
        w_kk[chan:2 * chan, h * LANES + head_dim:h * LANES + 2 * head_dim] = wide
    row = lax.broadcasted_iota(jnp.int32, (LANES - 2 * head_dim, 2 * LANES), 0)
    tail_scr[0:LANES - 2 * head_dim] = jnp.where(row < len(FILL_PARTS), 1.0, 0.0).astype(BF16)
    tail_scr[LANES - 2 * head_dim:] = jnp.concatenate([eye, eye], axis=1)
    lane = lax.broadcasted_iota(jnp.int32, (LANES, LANES), 1)
    part = jnp.zeros((LANES, LANES), F32)
    for n, f in enumerate(FILL_PARTS):
        part = jnp.where(lane == 2 * head_dim + n, f, part)
    keep = mask_ref[...].astype(F32)
    for n in range(rows // LANES):
        masked = jnp.broadcast_to(keep[n:n + 1], (LANES, LANES)).T
        fill_scr[n * LANES:(n + 1) * LANES] = jnp.where(masked > 0.5, 0.0, part).astype(BF16)
    q_scr[...] = jnp.zeros_like(q_scr)

    barrier = pltpu.get_barrier_semaphore()
    for s in range(1, n_row):
        pl.semaphore_signal(barrier, inc=1, device_id={'row': row_at(s)}, device_id_type=MESH)
    for s in range(1, n_col):
        pl.semaphore_signal(barrier, inc=1, device_id={'col': col_at(s)}, device_id_type=MESH)
    pl.semaphore_wait(barrier, n_row + n_col - 2)

    def send_group(c, lo=0, n=block):
        for s in range(1, n_row):
            to = row_at(s)
            pltpu.make_async_remote_copy(
                src_ref=z_ref.at[lo:lo + n, pl.ds(pl.multiple_of(to * share + c * GROUP, GROUP), GROUP), :],
                dst_ref=zin.at[c, pl.ds(pl.multiple_of(me * block + lo, 16), n)], send_sem=zsend_sem.at[s], recv_sem=zin_sem.at[c],
                device_id={'row': to}, device_id_type=MESH).start()
        pltpu.make_async_copy(z_ref.at[lo:lo + n, pl.ds(pl.multiple_of(me * share + c * GROUP, GROUP), GROUP), :],
                              zin.at[c, pl.ds(pl.multiple_of(me * block + lo, 16), n)], zin_sem.at[c]).start()

    early = block * 2 // 3
    send_group(0, 0, early)

    per = 8

    def own_bias(t, _):
        for u in range(per):
            k = t * per + u
            a = layer_norm(zown[k].astype(F32), gamma, beta).astype(BF16)
            for half, lo in enumerate((0, cols - LANES)):
                b_scr[pl.ds(half * 8 * block + k, 8, stride=block), :] = lax.dot_general(
                    w_b_t[...], a[lo:lo + LANES], NT, preferred_element_type=F32)
        return 0

    for q in range(4):
        own[q].wait()
        lax.fori_loop(q * (block // 4 // per), (q + 1) * (block // 4 // per), own_bias, 0)

    low = lower_half((block, LANES))
    def own_part(half, h):
        return b_scr[half * 8 * block + h * block:half * 8 * block + (h + 1) * block, :]

    for h in range(heads):
        brecv[my_col, me, h] = own_part(0, h).astype(BF16)
    for h in range(0, heads, 2):
        brecv[my_col, me, heads + h // 2] = jnp.where(low, swap_half(own_part(1, h)), own_part(1, h + 1)).astype(BF16)

    def tile(c, r):
        return brecv.at[c, r]

    def to_chip(d):
        to = row_at(2 * d)
        return pltpu.make_async_remote_copy(src_ref=tile(my_col, me), dst_ref=tile(my_col, me), send_sem=bxs_sem.at[d],
                                            recv_sem=bx_sem.at[d], device_id={'row': to}, device_id_type=MESH)

    def line(d):
        return row_at(n_row - 2 * d)

    def to_col(e, d):
        t = tile(my_col, line(d))
        return pltpu.make_async_remote_copy(src_ref=t, dst_ref=t, send_sem=bys_sem.at[e, d], recv_sem=by_sem.at[e, d],
                                            device_id={'col': col_at(e)}, device_id_type=MESH)

    def relay(d):
        e = 1 if d < n_chip // 2 else n_col - 1
        t = tile(col_at(n_col - e), line(d))
        return pltpu.make_async_remote_copy(src_ref=t, dst_ref=t, send_sem=bys_sem.at[2, d], recv_sem=by_sem.at[2, d],
                                            device_id={'col': col_at(e)}, device_id_type=MESH)

    def to_mate(e, d):
        t = tile(col_at(n_col - e), line(d))
        return pltpu.make_async_remote_copy(src_ref=t, dst_ref=t, send_sem=bds_sem.at[e, d], recv_sem=bd_sem.at[e, d],
                                            device_id={'row': mate}, device_id_type=MESH)

    near = (1, n_col - 1)

    def forward(d):
        for e in near:
            to_col(e, d).start()
        to_mate(0, d).start()

    for d in range(1, n_chip):
        to_chip(d).start()
    forward(0)

    def widen(col):
        def rows_of(r, _, c):
            at = pl.ds(pl.multiple_of(r * block, block), block)
            first = c * cols // LANES
            for h in range(heads):
                if c % 2 == 0:
                    bias_scr[h, first, at] = brecv[c, r, h]
                    b = brecv[c, r, heads + h // 2]
                    if h % 2:
                        b = swap_half(b.astype(F32)).astype(BF16)
                    bias_scr[h, first + 1, at, 0:HALF] = b[:, 0:HALF]
                else:
                    a = swap_half(brecv[c, r, h].astype(F32))
                    b = brecv[c, r, heads + h // 2].astype(F32)
                    b = b if h % 2 else swap_half(b)
                    bias_scr[h, first, at, HALF:LANES] = a.astype(BF16)[:, HALF:LANES]
                    bias_scr[h, first + 1, at] = jnp.where(low, a, b).astype(BF16)
            return 0

        for c in range(n_col):
            @pl.when(col == c)
            def _():
                lax.fori_loop(0, n_row, functools.partial(rows_of, c=c), 0)

    def arrived(c):
        pltpu.make_async_copy(zin.at[c], zin.at[c], zin_sem.at[c]).wait()

    def prepare(c):
        norm_group(zin, c, gamma, beta, a_scr)
        project_group(rows, a_scr, w_kk, w_qvg_t, fill_scr, k_scr, q_scr, v_scr, g_scr, head_dim)

    for d in sorted(range(1, n_chip), key=lambda d: min(d, n_chip - d)):
        to_chip(d).wait_recv()
        forward(d)
    send_group(0, early, block - early)
    for d in range(n_chip):
        for e in near:
            to_col(e, d).wait_recv()
            to_mate(e, d).start()
        relay(d).start()
    arrived(0)
    send_group(1)
    prepare(0)
    for e in (0,) + near:
        for d in range(n_chip):
            to_mate(e, d).wait_recv()

    def widen_near(t, _):
        widen(lax.rem(my_col + t + t // 2, n_col))
        return 0

    lax.fori_loop(0, 3, widen_near, 0)

    def far_to_mate():
        for d in range(n_chip):
            relay(d).wait_recv()
            to_mate(2, d).start()

    def far_ready():
        for d in range(n_chip):
            to_mate(2, d).wait_recv()
        widen(col_at(2))

    n_block = rows // LANES
    n_pair = GROUP // 2
    per_block = n_pair // UNROLL

    def group(c, _):
        first = jnp.where(c == 0, (my_col + 1) // 2, me // 2)

        def block_at(b):
            return lax.rem(b // 2 + first, n_block // 2) * 2 + lax.rem(b, 2)

        def where(u):
            return lax.rem(u, n_pair), block_at(u // n_pair)

        for h in range(heads):
            pair, ib = where(0)
            scores(pair, ib, h, rows, tail_scr, bias_scr, k_scr, q_scr, s_scr, top_scr)

        def one_block(b, _):
            def one(u, _):
                @pl.when((c == 0) & (u == (GROUP // 2 - 2) // UNROLL))
                def _():
                    far_to_mate()

                @pl.when((c == 0) & (u == (GROUP - 2) // UNROLL))
                def _():
                    far_ready()

                for v in range(UNROLL):
                    pair, ib = where(u * UNROLL + v)
                    npair, nib = where(jnp.minimum(u * UNROLL + v + 1, n_pair * n_block - 1))
                    for h in range(heads):
                        soft_and_next(pair, ib, npair, nib, h, rows, tail_scr, bias_scr, k_scr, q_scr, v_scr, g_scr, s_scr, top_scr, o_scr)
                return 0

            lax.fori_loop(b * per_block, (b + 1) * per_block, one, 0)
            lo = pl.multiple_of(block_at(b) * LANES, LANES)

            for j in range(GROUP):
                gated = o_scr[j, :, :, pl.ds(lo, LANES)].reshape(heads * head_dim, LANES)
                a_scr[pl.ds(lo * GROUP + j, LANES, stride=GROUP), :] = lax.dot_general(gated, w_o[...], TN, preferred_element_type=F32)

            def finish(t, _):
                at = pl.multiple_of(lo + t * HALF, HALF)
                upd = a_scr[pl.ds(pl.multiple_of(at * GROUP, HALF * GROUP), HALF * GROUP), :].reshape(HALF, GROUP, chan)
                zin[c, pl.ds(at, HALF)] = (zin[c, pl.ds(at, HALF)].astype(F32) + upd).astype(BF16)
                return 0

            lax.fori_loop(0, LANES // HALF, finish, 0)

            def send(t, _):
                seg = lo // PIECE + t
                to = seg // (block // PIECE)
                off = lax.rem(seg, block // PIECE) * PIECE
                src = zin.at[c, pl.ds(pl.multiple_of(seg * PIECE, PIECE), PIECE)]
                dst = out_ref.at[pl.ds(pl.multiple_of(off, PIECE), PIECE), pl.ds(pl.multiple_of(me * share + c * GROUP, GROUP), GROUP), :]

                @pl.when(to == me)
                def _():
                    pltpu.make_async_copy(src, dst, out_sem).start()

                @pl.when(to != me)
                def _():
                    pltpu.make_async_remote_copy(src_ref=src, dst_ref=dst, send_sem=osend_sem, recv_sem=out_sem,
                                                 device_id={'row': to}, device_id_type=MESH).start()
                return 0

            lax.fori_loop(0, LANES // PIECE, send, 0)
            return 0

        lax.fori_loop(0, n_block, one_block, 0)

        @pl.when(c < n_group - 1)
        def _():
            arrived(c + 1)

            @pl.when(c < n_group - 2)
            def _():
                send_group(c + 2)

            prepare(c + 1)
        return 0

    lax.fori_loop(0, n_group, group, 0)

    for s in range(1, n_row):
        pltpu.make_async_copy(z_ref.at[:, 0:share, :], z_ref.at[:, 0:share, :], zsend_sem.at[s]).wait()
    for d in range(1, n_chip):
        to_chip(d).wait_send()
    for d in range(n_chip):
        for e in near:
            to_col(e, d).wait_send()
        relay(d).wait_send()
        for e in range(n_col):
            to_mate(e, d).wait_send()
    pltpu.make_async_copy(zin.at[:, 0:rows - block], zin.at[:, 0:rows - block], osend_sem).wait()
    pltpu.make_async_copy(z_ref, out_ref, out_sem).wait()


def run(n_row, n_col, z, mask, gamma, beta, w_q, w_k, w_v, w_b, w_g, w_o):
    block, cols, chan = z.shape
    rows, share, proj = block * n_row, cols // n_row, w_k.shape[1]
    heads = w_b.shape[0]
    n_group, n_chip, head_dim = share // GROUP, n_row // 2, proj // heads
    vmem = pl.BlockSpec(memory_space=pltpu.VMEM)
    hbm = pl.BlockSpec(memory_space=pl.ANY)
    dma = pltpu.SemaphoreType.DMA
    return pl.pallas_call(
        functools.partial(kernel, n_row, n_col, heads),
        out_shape=jax.ShapeDtypeStruct(z.shape, BF16),
        in_specs=[hbm] + [vmem] * 9,
        out_specs=hbm,
        scratch_shapes=[
            pltpu.VMEM((3 * proj, chan), BF16),
            pltpu.VMEM((8, chan), BF16),
            pltpu.VMEM((2 * chan, heads * LANES), BF16),
            pltpu.VMEM((2 * LANES - 2 * head_dim, 2 * LANES), BF16),
            pltpu.VMEM((rows, LANES), BF16),
            pltpu.VMEM((block, cols, chan), BF16),
            pltpu.VMEM((n_group, rows, GROUP, chan), BF16),
            pltpu.VMEM((n_col, n_row, heads + heads // 2, block, LANES), BF16),
            pltpu.VMEM((2 * 8 * block, LANES), F32),
            pltpu.VMEM((rows * GROUP, chan), F32),
            pltpu.VMEM((GROUP // 2, heads, rows, LANES), BF16),
            pltpu.VMEM((GROUP // 2, heads, rows // LANES, 2 * head_dim, 2 * LANES), BF16),
            pltpu.VMEM((GROUP // 2, heads, 2 * head_dim, rows), BF16),
            pltpu.VMEM((GROUP, heads, head_dim, rows), F32),
            pltpu.VMEM((heads, rows // LANES, rows, LANES), BF16),
            pltpu.VMEM((heads, rows, BLOCK), F32),
            pltpu.VMEM((heads, 1, BLOCK), F32),
            pltpu.VMEM((GROUP, heads, head_dim, rows), BF16),
            dma((4,)), dma((n_group,)), dma((n_row,)), dma((n_chip,)), dma((n_chip,)), dma((n_col, n_chip)), dma((n_col, n_chip)),
            dma((n_col, n_chip)), dma((n_col, n_chip)), dma, dma,
        ],
        compiler_params=pltpu.CompilerParams(vmem_limit_bytes=62 * 1024 * 1024, collective_id=0, has_side_effects=True),
        name="triangle",
    )(z, mask, gamma, beta, w_q, w_k, w_v, w_b, w_g, w_o)


def solution(mesh):
    n_row, n_col = mesh.shape['row'], mesh.shape['col']

    def body(pair_tile, res_mask, ln_gamma, ln_beta, w_q, w_k, w_v, w_b, w_g, w_o):
        return run(n_row, n_col, pair_tile, res_mask.reshape(-1, LANES), ln_gamma[None], ln_beta[None], w_q, w_k, w_v, w_b.T, w_g, w_o)

    tile_spec = P(('data', 'row'), 'col', None)
    return jax.shard_map(body, mesh=mesh, in_specs=(tile_spec, P('data'), P(), P(), P(), P(), P(), P(), P(), P()), out_specs=tile_spec, check_vma=False)
```

```python
import functools
import math
import jax
import jax.numpy as jnp
from jax import lax
from jax.experimental import pallas as pl
from jax.experimental.pallas import tpu as pltpu
from jax.sharding import PartitionSpec as P

LN_EPS = 1e-5
FILL_PARTS = (-998244352.0, -1753088.0, -2560.0)
assert sum(FILL_PARTS) == -1e9
GROUP = 8
BLOCK = 256
PIECE = 32
KC = 384
LANES = 128
HALF = 64
UNROLL = 2
F32 = jnp.float32
BF16 = jnp.bfloat16
NT = (((1,), (1,)), ((), ()))
TN = (((0,), (0,)), ((), ()))
MESH = pl.DeviceIdType.MESH


def layer_norm(z, gamma, beta):
    mean = jnp.mean(z, axis=-1, keepdims=True)
    centred = z - mean
    variance = jnp.mean(centred * centred, axis=-1, keepdims=True)
    return centred * lax.rsqrt(variance + LN_EPS) * gamma + beta


def norm_group(zin, c, gamma, beta, a_scr, step=64):
    rows = zin.shape[1]

    def one(t, _):
        lo = pl.multiple_of(t * step, step)
        a = layer_norm(zin[c, pl.ds(lo, step)].astype(F32), gamma, beta)
        a_scr[pl.ds(pl.multiple_of(lo * GROUP, step * GROUP), step * GROUP), :] = a.reshape(step * GROUP, a.shape[-1])
        return 0

    lax.fori_loop(0, rows // step, one, 0)


def project_group(rows, a_scr, w_kk, w_qvg_t, fill_scr, k_scr, q_scr, v_scr, g_scr, head_dim):
    proj = w_qvg_t.shape[0] // 3
    heads = proj // head_dim

    def one(pair, _):
        cols = []
        for side in range(2):
            j = 2 * pair + side
            a = a_scr[pl.ds(j, rows, stride=GROUP), :].astype(BF16)
            cols.append(a)
            for lo in range(0, rows, 2 * LANES):
                t = lax.dot_general(w_qvg_t[...], a[lo:lo + 2 * LANES], NT, preferred_element_type=F32)
                for h in range(heads):
                    hs = slice(h * head_dim, (h + 1) * head_dim)
                    q = (t[hs] * (1.0 / math.sqrt(head_dim))).astype(BF16)
                    here = slice(side * head_dim, (side + 1) * head_dim)
                    for n in range(2):
                        q_scr[pair, h, lo // LANES + n, here, side * LANES:(side + 1) * LANES] = q[:, n * LANES:(n + 1) * LANES]
                    v_scr[pair, h, here, lo:lo + 2 * LANES] = t[proj:2 * proj][hs].astype(BF16)
                    g_scr[j, h, :, lo:lo + 2 * LANES] = jax.nn.sigmoid(t[2 * proj:][hs])
        a = jnp.concatenate(cols, axis=1)
        for lo in range(0, rows, 2 * LANES):
            fill = fill_scr[lo:lo + 2 * LANES]
            for h in range(0, heads, 2):
                k = jnp.dot(a[lo:lo + 2 * LANES], w_kk[:, h * LANES:(h + 2) * LANES], preferred_element_type=F32).astype(BF16)
                k_scr[pair, h, lo:lo + 2 * LANES] = k[:, 0:LANES] + fill
                k_scr[pair, h + 1, lo:lo + 2 * LANES] = k[:, LANES:2 * LANES] + fill
        return 0

    lax.fori_loop(0, GROUP // 2, one, 0)


def right_side(pair, h, ib, q_scr, tail_scr):
    return jnp.concatenate([q_scr[pair, h, ib], tail_scr[...]], axis=0)


def score_chunk(pair, h, ib, kc, right, bias_scr, k_scr):
    left = jnp.concatenate([k_scr[pair, h, kc:kc + KC], bias_scr[h, ib, kc:kc + KC]], axis=1)
    return jnp.dot(left, right, preferred_element_type=F32)


def fold8(x, op):
    return op(x.reshape(x.shape[0] // 8, 8, x.shape[1]), axis=0)


def scores(pair, ib, h, rows, tail_scr, bias_scr, k_scr, q_scr, s_scr, top_scr):
    top = None
    right = right_side(pair, h, ib, q_scr, tail_scr)
    for kc in range(0, rows, KC):
        s = score_chunk(pair, h, ib, kc, right, bias_scr, k_scr)
        s_scr[h, kc:kc + KC] = s
        part = fold8(s, jnp.max)
        top = part if top is None else jnp.maximum(top, part)
    top_scr[h] = jnp.max(top, axis=0, keepdims=True)


def soft_and_next(pair, ib, npair, nib, h, rows, tail_scr, bias_scr, k_scr, q_scr, v_scr, g_scr, s_scr, top_scr, o_scr):
    head_dim = g_scr.shape[2]
    top = top_scr[h]
    total = acc = ntop = None
    right = right_side(npair, h, nib, q_scr, tail_scr)
    for kc in range(0, rows, KC):
        p = jnp.exp(s_scr[h, kc:kc + KC] - top)
        part = fold8(p, jnp.sum)
        total = part if total is None else total + part
        o = jnp.dot(v_scr[pair, h, :, kc:kc + KC], p.astype(BF16), preferred_element_type=F32)
        acc = o if acc is None else acc + o
        s = score_chunk(npair, h, nib, kc, right, bias_scr, k_scr)
        s_scr[h, kc:kc + KC] = s
        part = fold8(s, jnp.max)
        ntop = part if ntop is None else jnp.maximum(ntop, part)
    top_scr[h] = jnp.max(ntop, axis=0, keepdims=True)
    total = jnp.sum(total, axis=0, keepdims=True)
    at = pl.ds(pl.multiple_of(ib * LANES, LANES), LANES)
    for side in range(2):
        lanes = slice(side * LANES, (side + 1) * LANES)
        o = acc[side * head_dim:(side + 1) * head_dim, lanes] / total[:, lanes]
        o_scr[2 * pair + side, h, :, at] = (g_scr[2 * pair + side, h, :, at] * o).astype(BF16)


def swap_half(x):
    return pltpu.roll(x, HALF, 1)


def lower_half(shape):
    return lax.broadcasted_iota(jnp.int32, shape, len(shape) - 1) < HALF


def kernel(n_row, n_col, heads, z_ref, mask_ref, gamma_ref, beta_ref, w_q, w_k, w_v, w_b, w_g, w_o, out_ref,
           w_qvg_t, w_b_t, w_kk, tail_scr, fill_scr, zown, zin, brecv, b_scr, a_scr, k_scr, q_scr, v_scr, g_scr, bias_scr, s_scr, top_scr, o_scr,
           own_sem, zin_sem, zsend_sem, bx_sem, bxs_sem, by_sem, bys_sem, bd_sem, bds_sem, out_sem, osend_sem):
    block, cols, chan = z_ref.shape
    rows = block * n_row
    share = cols // n_row
    n_group = share // GROUP
    head_dim = w_k.shape[1] // heads
    n_chip = n_row // 2
    me = lax.axis_index('row')
    my_col = lax.axis_index('col')
    mate = me + 1 - 2 * lax.rem(me, 2)
    gamma, beta = gamma_ref[...], beta_ref[...]

    def row_at(s):
        return lax.rem(me + s, n_row)

    def col_at(s):
        return lax.rem(my_col + s, n_col)

    own = [pltpu.make_async_copy(z_ref.at[pl.ds(q * (block // 4), block // 4)], zown.at[pl.ds(q * (block // 4), block // 4)], own_sem.at[q]) for q in range(4)]
    for cp in own:
        cp.start()

    proj = heads * head_dim
    for n, w in enumerate((w_q, w_v, w_g)):
        w_qvg_t[n * proj:(n + 1) * proj] = w[...].astype(F32).T.astype(BF16)
    eye = (lax.broadcasted_iota(jnp.int32, (chan, chan), 0) == lax.broadcasted_iota(jnp.int32, (chan, chan), 1)).astype(BF16)
    w_b_t[...] = jnp.zeros_like(w_b_t)
    w_b_t[0:heads] = w_b[...]
    w_kk[...] = jnp.zeros_like(w_kk)
    for h in range(heads):
        wide = w_k[:, h * head_dim:(h + 1) * head_dim]
        w_kk[0:chan, h * LANES:h * LANES + head_dim] = wide
        w_kk[chan:2 * chan, h * LANES + head_dim:h * LANES + 2 * head_dim] = wide
    row = lax.broadcasted_iota(jnp.int32, (LANES - 2 * head_dim, 2 * LANES), 0)
    tail_scr[0:LANES - 2 * head_dim] = jnp.where(row < len(FILL_PARTS), 1.0, 0.0).astype(BF16)
    tail_scr[LANES - 2 * head_dim:] = jnp.concatenate([eye, eye], axis=1)
    lane = lax.broadcasted_iota(jnp.int32, (LANES, LANES), 1)
    part = jnp.zeros((LANES, LANES), F32)
    for n, f in enumerate(FILL_PARTS):
        part = jnp.where(lane == 2 * head_dim + n, f, part)
    keep = mask_ref[...].astype(F32)
    for n in range(rows // LANES):
        masked = jnp.broadcast_to(keep[n:n + 1], (LANES, LANES)).T
        fill_scr[n * LANES:(n + 1) * LANES] = jnp.where(masked > 0.5, 0.0, part).astype(BF16)
    q_scr[...] = jnp.zeros_like(q_scr)

    barrier = pltpu.get_barrier_semaphore()
    for s in range(1, n_row):
        pl.semaphore_signal(barrier, inc=1, device_id={'row': row_at(s)}, device_id_type=MESH)
    for s in range(1, n_col):
        pl.semaphore_signal(barrier, inc=1, device_id={'col': col_at(s)}, device_id_type=MESH)
    pl.semaphore_wait(barrier, n_row + n_col - 2)

    def send_group(c, lo=0, n=block):
        for s in range(1, n_row):
            to = row_at(s)
            pltpu.make_async_remote_copy(
                src_ref=z_ref.at[lo:lo + n, pl.ds(pl.multiple_of(to * share + c * GROUP, GROUP), GROUP), :],
                dst_ref=zin.at[c, pl.ds(pl.multiple_of(me * block + lo, 16), n)], send_sem=zsend_sem.at[s], recv_sem=zin_sem.at[c],
                device_id={'row': to}, device_id_type=MESH).start()
        pltpu.make_async_copy(z_ref.at[lo:lo + n, pl.ds(pl.multiple_of(me * share + c * GROUP, GROUP), GROUP), :],
                              zin.at[c, pl.ds(pl.multiple_of(me * block + lo, 16), n)], zin_sem.at[c]).start()

    early = block * 2 // 3
    send_group(0, 0, early)

    per = 8

    def own_bias(t, _):
        for u in range(per):
            k = t * per + u
            a = layer_norm(zown[k].astype(F32), gamma, beta).astype(BF16)
            for half, lo in enumerate((0, cols - LANES)):
                b_scr[pl.ds(half * 8 * block + k, 8, stride=block), :] = lax.dot_general(
                    w_b_t[...], a[lo:lo + LANES], NT, preferred_element_type=F32)
        return 0

    for q in range(4):
        own[q].wait()
        lax.fori_loop(q * (block // 4 // per), (q + 1) * (block // 4 // per), own_bias, 0)

    low = lower_half((block, LANES))
    def own_part(half, h):
        return b_scr[half * 8 * block + h * block:half * 8 * block + (h + 1) * block, :]

    for h in range(heads):
        brecv[my_col, me, h] = own_part(0, h).astype(BF16)
    for h in range(0, heads, 2):
        brecv[my_col, me, heads + h // 2] = jnp.where(low, swap_half(own_part(1, h)), own_part(1, h + 1)).astype(BF16)

    def tile(c, r):
        return brecv.at[c, r]

    def to_chip(d):
        to = row_at(2 * d)
        return pltpu.make_async_remote_copy(src_ref=tile(my_col, me), dst_ref=tile(my_col, me), send_sem=bxs_sem.at[d],
                                            recv_sem=bx_sem.at[d], device_id={'row': to}, device_id_type=MESH)

    def line(d):
        return row_at(n_row - 2 * d)

    def to_col(e, d):
        t = tile(my_col, line(d))
        return pltpu.make_async_remote_copy(src_ref=t, dst_ref=t, send_sem=bys_sem.at[e, d], recv_sem=by_sem.at[e, d],
                                            device_id={'col': col_at(e)}, device_id_type=MESH)

    def relay(d):
        e = 1 if d < n_chip // 2 else n_col - 1
        t = tile(col_at(n_col - e), line(d))
        return pltpu.make_async_remote_copy(src_ref=t, dst_ref=t, send_sem=bys_sem.at[2, d], recv_sem=by_sem.at[2, d],
                                            device_id={'col': col_at(e)}, device_id_type=MESH)

    def to_mate(e, d):
        t = tile(col_at(n_col - e), line(d))
        return pltpu.make_async_remote_copy(src_ref=t, dst_ref=t, send_sem=bds_sem.at[e, d], recv_sem=bd_sem.at[e, d],
                                            device_id={'row': mate}, device_id_type=MESH)

    near = (1, n_col - 1)

    def forward(d):
        for e in near:
            to_col(e, d).start()
        to_mate(0, d).start()

    for d in range(1, n_chip):
        to_chip(d).start()
    forward(0)

    def widen(col):
        def rows_of(r, _, c):
            at = pl.ds(pl.multiple_of(r * block, block), block)
            first = c * cols // LANES
            for h in range(heads):
                if c % 2 == 0:
                    bias_scr[h, first, at] = brecv[c, r, h]
                    b = brecv[c, r, heads + h // 2]
                    if h % 2:
                        b = swap_half(b.astype(F32)).astype(BF16)
                    bias_scr[h, first + 1, at, 0:HALF] = b[:, 0:HALF]
                else:
                    a = swap_half(brecv[c, r, h].astype(F32))
                    b = brecv[c, r, heads + h // 2].astype(F32)
                    b = b if h % 2 else swap_half(b)
                    bias_scr[h, first, at, HALF:LANES] = a.astype(BF16)[:, HALF:LANES]
                    bias_scr[h, first + 1, at] = jnp.where(low, a, b).astype(BF16)
            return 0

        for c in range(n_col):
            @pl.when(col == c)
            def _():
                lax.fori_loop(0, n_row, functools.partial(rows_of, c=c), 0)

    def arrived(c):
        pltpu.make_async_copy(zin.at[c], zin.at[c], zin_sem.at[c]).wait()

    def prepare(c):
        norm_group(zin, c, gamma, beta, a_scr)
        project_group(rows, a_scr, w_kk, w_qvg_t, fill_scr, k_scr, q_scr, v_scr, g_scr, head_dim)

    for d in sorted(range(1, n_chip), key=lambda d: min(d, n_chip - d)):
        to_chip(d).wait_recv()
        forward(d)
    send_group(0, early, block - early)
    for d in range(n_chip):
        to_mate(0, d).wait_recv()
    widen(my_col)
    arrived(0)
    send_group(1)
    norm_group(zin, 0, gamma, beta, a_scr)
    for d in range(n_chip):
        for e in near:
            to_col(e, d).wait_recv()
            to_mate(e, d).start()
        relay(d).start()
    project_group(rows, a_scr, w_kk, w_qvg_t, fill_scr, k_scr, q_scr, v_scr, g_scr, head_dim)
    for e in near:
        for d in range(n_chip):
            to_mate(e, d).wait_recv()

    def widen_near(t, _):
        widen(lax.rem(my_col + 1 + t * (n_col - 2), n_col))
        return 0

    lax.fori_loop(0, 2, widen_near, 0)

    def far_to_mate():
        for d in range(n_chip):
            relay(d).wait_recv()
            to_mate(2, d).start()

    def far_ready():
        for d in range(n_chip):
            to_mate(2, d).wait_recv()
        widen(col_at(2))

    n_block = rows // LANES
    n_pair = GROUP // 2
    per_block = n_pair // UNROLL

    def group(c, _):
        first = jnp.where(c == 0, (my_col + 1) // 2, me // 2)

        def block_at(b):
            return lax.rem(b // 2 + first, n_block // 2) * 2 + lax.rem(b, 2)

        def where(u):
            return lax.rem(u, n_pair), block_at(u // n_pair)

        for h in range(heads):
            pair, ib = where(0)
            scores(pair, ib, h, rows, tail_scr, bias_scr, k_scr, q_scr, s_scr, top_scr)

        def one_block(b, _):
            def one(u, _):
                @pl.when((c == 0) & (u == (GROUP // 2 - 2) // UNROLL))
                def _():
                    far_to_mate()

                @pl.when((c == 0) & (u == (GROUP - 2) // UNROLL))
                def _():
                    far_ready()

                for v in range(UNROLL):
                    pair, ib = where(u * UNROLL + v)
                    npair, nib = where(jnp.minimum(u * UNROLL + v + 1, n_pair * n_block - 1))
                    for h in range(heads):
                        soft_and_next(pair, ib, npair, nib, h, rows, tail_scr, bias_scr, k_scr, q_scr, v_scr, g_scr, s_scr, top_scr, o_scr)
                return 0

            lax.fori_loop(b * per_block, (b + 1) * per_block, one, 0)
            lo = pl.multiple_of(block_at(b) * LANES, LANES)

            for j in range(GROUP):
                gated = o_scr[j, :, :, pl.ds(lo, LANES)].reshape(heads * head_dim, LANES)
                a_scr[pl.ds(lo * GROUP + j, LANES, stride=GROUP), :] = lax.dot_general(gated, w_o[...], TN, preferred_element_type=F32)

            def finish(t, _):
                at = pl.multiple_of(lo + t * HALF, HALF)
                upd = a_scr[pl.ds(pl.multiple_of(at * GROUP, HALF * GROUP), HALF * GROUP), :].reshape(HALF, GROUP, chan)
                zin[c, pl.ds(at, HALF)] = (zin[c, pl.ds(at, HALF)].astype(F32) + upd).astype(BF16)
                return 0

            lax.fori_loop(0, LANES // HALF, finish, 0)

            def send(t, _):
                seg = lo // PIECE + t
                to = seg // (block // PIECE)
                off = lax.rem(seg, block // PIECE) * PIECE
                src = zin.at[c, pl.ds(pl.multiple_of(seg * PIECE, PIECE), PIECE)]
                dst = out_ref.at[pl.ds(pl.multiple_of(off, PIECE), PIECE), pl.ds(pl.multiple_of(me * share + c * GROUP, GROUP), GROUP), :]

                @pl.when(to == me)
                def _():
                    pltpu.make_async_copy(src, dst, out_sem).start()

                @pl.when(to != me)
                def _():
                    pltpu.make_async_remote_copy(src_ref=src, dst_ref=dst, send_sem=osend_sem, recv_sem=out_sem,
                                                 device_id={'row': to}, device_id_type=MESH).start()
                return 0

            lax.fori_loop(0, LANES // PIECE, send, 0)
            return 0

        lax.fori_loop(0, n_block, one_block, 0)

        @pl.when(c < n_group - 1)
        def _():
            arrived(c + 1)

            @pl.when(c < n_group - 2)
            def _():
                send_group(c + 2)

            prepare(c + 1)
        return 0

    lax.fori_loop(0, n_group, group, 0)

    for s in range(1, n_row):
        pltpu.make_async_copy(z_ref.at[:, 0:share, :], z_ref.at[:, 0:share, :], zsend_sem.at[s]).wait()
    for d in range(1, n_chip):
        to_chip(d).wait_send()
    for d in range(n_chip):
        for e in near:
            to_col(e, d).wait_send()
        relay(d).wait_send()
        for e in range(n_col):
            to_mate(e, d).wait_send()
    pltpu.make_async_copy(zin.at[:, 0:rows - block], zin.at[:, 0:rows - block], osend_sem).wait()
    pltpu.make_async_copy(z_ref, out_ref, out_sem).wait()


def run(n_row, n_col, z, mask, gamma, beta, w_q, w_k, w_v, w_b, w_g, w_o):
    block, cols, chan = z.shape
    rows, share, proj = block * n_row, cols // n_row, w_k.shape[1]
    heads = w_b.shape[0]
    n_group, n_chip, head_dim = share // GROUP, n_row // 2, proj // heads
    vmem = pl.BlockSpec(memory_space=pltpu.VMEM)
    hbm = pl.BlockSpec(memory_space=pl.ANY)
    dma = pltpu.SemaphoreType.DMA
    return pl.pallas_call(
        functools.partial(kernel, n_row, n_col, heads),
        out_shape=jax.ShapeDtypeStruct(z.shape, BF16),
        in_specs=[hbm] + [vmem] * 9,
        out_specs=hbm,
        scratch_shapes=[
            pltpu.VMEM((3 * proj, chan), BF16),
            pltpu.VMEM((8, chan), BF16),
            pltpu.VMEM((2 * chan, heads * LANES), BF16),
            pltpu.VMEM((2 * LANES - 2 * head_dim, 2 * LANES), BF16),
            pltpu.VMEM((rows, LANES), BF16),
            pltpu.VMEM((block, cols, chan), BF16),
            pltpu.VMEM((n_group, rows, GROUP, chan), BF16),
            pltpu.VMEM((n_col, n_row, heads + heads // 2, block, LANES), BF16),
            pltpu.VMEM((2 * 8 * block, LANES), F32),
            pltpu.VMEM((rows * GROUP, chan), F32),
            pltpu.VMEM((GROUP // 2, heads, rows, LANES), BF16),
            pltpu.VMEM((GROUP // 2, heads, rows // LANES, 2 * head_dim, 2 * LANES), BF16),
            pltpu.VMEM((GROUP // 2, heads, 2 * head_dim, rows), BF16),
            pltpu.VMEM((GROUP, heads, head_dim, rows), F32),
            pltpu.VMEM((heads, rows // LANES, rows, LANES), BF16),
            pltpu.VMEM((heads, rows, BLOCK), F32),
            pltpu.VMEM((heads, 1, BLOCK), F32),
            pltpu.VMEM((GROUP, heads, head_dim, rows), BF16),
            dma((4,)), dma((n_group,)), dma((n_row,)), dma((n_chip,)), dma((n_chip,)), dma((n_col, n_chip)), dma((n_col, n_chip)),
            dma((n_col, n_chip)), dma((n_col, n_chip)), dma, dma,
        ],
        compiler_params=pltpu.CompilerParams(vmem_limit_bytes=62 * 1024 * 1024, collective_id=0, has_side_effects=True),
        name="triangle",
    )(z, mask, gamma, beta, w_q, w_k, w_v, w_b, w_g, w_o)


def copy_out(x, pieces=8):
    step = x.shape[0] // pieces

    def body(x_ref, o_ref, buf, in_sem, out_sem):
        def part(n):
            return pl.ds(n * step, step)

        loads = [pltpu.make_async_copy(x_ref.at[part(n)], buf.at[part(n)], in_sem.at[n]) for n in range(pieces)]
        stores = [pltpu.make_async_copy(buf.at[part(n)], o_ref.at[part(n)], out_sem.at[n]) for n in range(pieces)]
        for load in loads:
            load.start()
        for load, store in zip(loads, stores):
            load.wait()
            store.start()
        for store in stores:
            store.wait()

    hbm = pl.BlockSpec(memory_space=pltpu.HBM)
    return pl.pallas_call(
        body,
        out_shape=jax.ShapeDtypeStruct(x.shape, x.dtype),
        in_specs=[hbm],
        out_specs=hbm,
        scratch_shapes=[pltpu.VMEM(x.shape, x.dtype), pltpu.SemaphoreType.DMA((pieces,)), pltpu.SemaphoreType.DMA((pieces,))],
        compiler_params=pltpu.CompilerParams(vmem_limit_bytes=62 * 1024 * 1024),
        name="copy_out",
    )(x)


def solution(mesh):
    n_row, n_col = mesh.shape['row'], mesh.shape['col']

    def body(pair_tile, res_mask, ln_gamma, ln_beta, w_q, w_k, w_v, w_b, w_g, w_o):
        out = run(n_row, n_col, pair_tile, res_mask.reshape(-1, LANES), ln_gamma[None], ln_beta[None], w_q, w_k, w_v, w_b.T, w_g, w_o)
        return copy_out(out)

    tile_spec = P(('data', 'row'), 'col', None)
    return jax.shard_map(body, mesh=mesh, in_specs=(tile_spec, P('data'), P(), P(), P(), P(), P(), P(), P(), P()), out_specs=tile_spec, check_vma=False)
```

```python
import functools
import math
import jax
import jax.numpy as jnp
from jax import lax
from jax.experimental import pallas as pl
from jax.experimental.pallas import tpu as pltpu
from jax.sharding import PartitionSpec as P

LN_EPS = 1e-5
FILL_PARTS = (-998244352.0, -1753088.0, -2560.0)
assert sum(FILL_PARTS) == -1e9
GROUP = 8
BLOCK = 256
PIECE = 32
KC = 384
LANES = 128
HALF = 64
UNROLL = 2
F32 = jnp.float32
BF16 = jnp.bfloat16
NT = (((1,), (1,)), ((), ()))
TN = (((0,), (0,)), ((), ()))
MESH = pl.DeviceIdType.MESH


def layer_norm(z, gamma, beta):
    mean = jnp.mean(z, axis=-1, keepdims=True)
    centred = z - mean
    variance = jnp.mean(centred * centred, axis=-1, keepdims=True)
    return centred * lax.rsqrt(variance + LN_EPS) * gamma + beta


def norm_group(zin, c, gamma, beta, a_scr, step=64):
    rows = zin.shape[1]

    def one(t, _):
        lo = pl.multiple_of(t * step, step)
        a = layer_norm(zin[c, pl.ds(lo, step)].astype(F32), gamma, beta)
        a_scr[pl.ds(pl.multiple_of(lo * GROUP, step * GROUP), step * GROUP), :] = a.reshape(step * GROUP, a.shape[-1])
        return 0

    lax.fori_loop(0, rows // step, one, 0)


def project_group(rows, a_scr, w_kk, w_qvg_t, fill_scr, k_scr, q_scr, v_scr, g_scr, head_dim):
    proj = w_qvg_t.shape[0] // 3
    heads = proj // head_dim

    def one(pair, _):
        cols = []
        for side in range(2):
            j = 2 * pair + side
            a = a_scr[pl.ds(j, rows, stride=GROUP), :].astype(BF16)
            cols.append(a)
            for lo in range(0, rows, 2 * LANES):
                t = lax.dot_general(w_qvg_t[...], a[lo:lo + 2 * LANES], NT, preferred_element_type=F32)
                for h in range(heads):
                    hs = slice(h * head_dim, (h + 1) * head_dim)
                    q = (t[hs] * (1.0 / math.sqrt(head_dim))).astype(BF16)
                    here = slice(side * head_dim, (side + 1) * head_dim)
                    for n in range(2):
                        q_scr[pair, h, lo // LANES + n, here, side * LANES:(side + 1) * LANES] = q[:, n * LANES:(n + 1) * LANES]
                    v_scr[pair, h, here, lo:lo + 2 * LANES] = t[proj:2 * proj][hs].astype(BF16)
                    g_scr[j, h, :, lo:lo + 2 * LANES] = jax.nn.sigmoid(t[2 * proj:][hs])
        a = jnp.concatenate(cols, axis=1)
        for lo in range(0, rows, 2 * LANES):
            fill = fill_scr[lo:lo + 2 * LANES]
            for h in range(0, heads, 2):
                k = jnp.dot(a[lo:lo + 2 * LANES], w_kk[:, h * LANES:(h + 2) * LANES], preferred_element_type=F32).astype(BF16)
                k_scr[pair, h, lo:lo + 2 * LANES] = k[:, 0:LANES] + fill
                k_scr[pair, h + 1, lo:lo + 2 * LANES] = k[:, LANES:2 * LANES] + fill
        return 0

    lax.fori_loop(0, GROUP // 2, one, 0)


def right_side(pair, h, ib, q_scr, tail_scr):
    return jnp.concatenate([q_scr[pair, h, ib], tail_scr[...]], axis=0)


def score_chunk(pair, h, ib, kc, right, bias_scr, k_scr):
    left = jnp.concatenate([k_scr[pair, h, kc:kc + KC], bias_scr[h, ib, kc:kc + KC]], axis=1)
    return jnp.dot(left, right, preferred_element_type=F32)


def fold8(x, op):
    return op(x.reshape(x.shape[0] // 8, 8, x.shape[1]), axis=0)


def scores(pair, ib, h, rows, tail_scr, bias_scr, k_scr, q_scr, s_scr, top_scr):
    top = None
    right = right_side(pair, h, ib, q_scr, tail_scr)
    for kc in range(0, rows, KC):
        s = score_chunk(pair, h, ib, kc, right, bias_scr, k_scr)
        s_scr[h, kc:kc + KC] = s
        part = fold8(s, jnp.max)
        top = part if top is None else jnp.maximum(top, part)
    top_scr[h] = jnp.max(top, axis=0, keepdims=True)


def soft_and_next(pair, ib, npair, nib, h, rows, tail_scr, bias_scr, k_scr, q_scr, v_scr, g_scr, s_scr, top_scr, o_scr):
    head_dim = g_scr.shape[2]
    top = top_scr[h]
    total = acc = ntop = None
    right = right_side(npair, h, nib, q_scr, tail_scr)
    for kc in range(0, rows, KC):
        p = jnp.exp(s_scr[h, kc:kc + KC] - top)
        part = fold8(p, jnp.sum)
        total = part if total is None else total + part
        o = jnp.dot(v_scr[pair, h, :, kc:kc + KC], p.astype(BF16), preferred_element_type=F32)
        acc = o if acc is None else acc + o
        s = score_chunk(npair, h, nib, kc, right, bias_scr, k_scr)
        s_scr[h, kc:kc + KC] = s
        part = fold8(s, jnp.max)
        ntop = part if ntop is None else jnp.maximum(ntop, part)
    top_scr[h] = jnp.max(ntop, axis=0, keepdims=True)
    total = jnp.sum(total, axis=0, keepdims=True)
    at = pl.ds(pl.multiple_of(ib * LANES, LANES), LANES)
    for side in range(2):
        lanes = slice(side * LANES, (side + 1) * LANES)
        o = acc[side * head_dim:(side + 1) * head_dim, lanes] / total[:, lanes]
        o_scr[2 * pair + side, h, :, at] = (g_scr[2 * pair + side, h, :, at] * o).astype(BF16)


def swap_half(x):
    return pltpu.roll(x, HALF, 1)


def lower_half(shape):
    return lax.broadcasted_iota(jnp.int32, shape, len(shape) - 1) < HALF


def kernel(n_row, n_col, heads, z_ref, mask_ref, gamma_ref, beta_ref, w_q, w_k, w_v, w_b, w_g, w_o, out_ref,
           w_qvg_t, w_b_t, w_kk, tail_scr, fill_scr, zown, zin, brecv, b_scr, a_scr, k_scr, q_scr, v_scr, g_scr, bias_scr, s_scr, top_scr, o_scr,
           own_sem, zin_sem, zsend_sem, bx_sem, bxs_sem, by_sem, bys_sem, bd_sem, bds_sem, out_sem, osend_sem):
    block, cols, chan = z_ref.shape
    rows = block * n_row
    share = cols // n_row
    n_group = share // GROUP
    head_dim = w_k.shape[1] // heads
    n_chip = n_row // 2
    me = lax.axis_index('row')
    my_col = lax.axis_index('col')
    mate = me + 1 - 2 * lax.rem(me, 2)
    gamma, beta = gamma_ref[...], beta_ref[...]

    def row_at(s):
        return lax.rem(me + s, n_row)

    def col_at(s):
        return lax.rem(my_col + s, n_col)

    own = [pltpu.make_async_copy(z_ref.at[pl.ds(q * (block // 4), block // 4)], zown.at[pl.ds(q * (block // 4), block // 4)], own_sem.at[q]) for q in range(4)]
    for cp in own:
        cp.start()

    proj = heads * head_dim
    for n, w in enumerate((w_q, w_v, w_g)):
        w_qvg_t[n * proj:(n + 1) * proj] = w[...].astype(F32).T.astype(BF16)
    eye = (lax.broadcasted_iota(jnp.int32, (chan, chan), 0) == lax.broadcasted_iota(jnp.int32, (chan, chan), 1)).astype(BF16)
    w_b_t[...] = jnp.zeros_like(w_b_t)
    w_b_t[0:heads] = w_b[...]
    w_kk[...] = jnp.zeros_like(w_kk)
    for h in range(heads):
        wide = w_k[:, h * head_dim:(h + 1) * head_dim]
        w_kk[0:chan, h * LANES:h * LANES + head_dim] = wide
        w_kk[chan:2 * chan, h * LANES + head_dim:h * LANES + 2 * head_dim] = wide
    row = lax.broadcasted_iota(jnp.int32, (LANES - 2 * head_dim, 2 * LANES), 0)
    tail_scr[0:LANES - 2 * head_dim] = jnp.where(row < len(FILL_PARTS), 1.0, 0.0).astype(BF16)
    tail_scr[LANES - 2 * head_dim:] = jnp.concatenate([eye, eye], axis=1)
    lane = lax.broadcasted_iota(jnp.int32, (LANES, LANES), 1)
    part = jnp.zeros((LANES, LANES), F32)
    for n, f in enumerate(FILL_PARTS):
        part = jnp.where(lane == 2 * head_dim + n, f, part)
    keep = mask_ref[...].astype(F32)
    for n in range(rows // LANES):
        masked = jnp.broadcast_to(keep[n:n + 1], (LANES, LANES)).T
        fill_scr[n * LANES:(n + 1) * LANES] = jnp.where(masked > 0.5, 0.0, part).astype(BF16)
    q_scr[...] = jnp.zeros_like(q_scr)

    barrier = pltpu.get_barrier_semaphore()
    for s in range(1, n_row):
        pl.semaphore_signal(barrier, inc=1, device_id={'row': row_at(s)}, device_id_type=MESH)
    for s in range(1, n_col):
        pl.semaphore_signal(barrier, inc=1, device_id={'col': col_at(s)}, device_id_type=MESH)
    pl.semaphore_wait(barrier, n_row + n_col - 2)

    def send_group(c, lo=0, n=block):
        for s in range(1, n_row):
            to = row_at(s)
            pltpu.make_async_remote_copy(
                src_ref=z_ref.at[lo:lo + n, pl.ds(pl.multiple_of(to * share + c * GROUP, GROUP), GROUP), :],
                dst_ref=zin.at[c, pl.ds(pl.multiple_of(me * block + lo, 16), n)], send_sem=zsend_sem.at[s], recv_sem=zin_sem.at[c],
                device_id={'row': to}, device_id_type=MESH).start()
        pltpu.make_async_copy(z_ref.at[lo:lo + n, pl.ds(pl.multiple_of(me * share + c * GROUP, GROUP), GROUP), :],
                              zin.at[c, pl.ds(pl.multiple_of(me * block + lo, 16), n)], zin_sem.at[c]).start()

    early = block * 2 // 3
    send_group(0, 0, early)

    per = 8

    def own_bias(t, _):
        for u in range(per):
            k = t * per + u
            a = layer_norm(zown[k].astype(F32), gamma, beta).astype(BF16)
            for half, lo in enumerate((0, cols - LANES)):
                b_scr[pl.ds(half * 8 * block + k, 8, stride=block), :] = lax.dot_general(
                    w_b_t[...], a[lo:lo + LANES], NT, preferred_element_type=F32)
        return 0

    for q in range(4):
        own[q].wait()
        lax.fori_loop(q * (block // 4 // per), (q + 1) * (block // 4 // per), own_bias, 0)

    low = lower_half((block, LANES))
    def own_part(half, h):
        return b_scr[half * 8 * block + h * block:half * 8 * block + (h + 1) * block, :]

    for h in range(heads):
        brecv[my_col, me, h] = own_part(0, h).astype(BF16)
    for h in range(0, heads, 2):
        brecv[my_col, me, heads + h // 2] = jnp.where(low, swap_half(own_part(1, h)), own_part(1, h + 1)).astype(BF16)

    def tile(c, r):
        return brecv.at[c, r]

    def to_chip(d):
        to = row_at(2 * d)
        return pltpu.make_async_remote_copy(src_ref=tile(my_col, me), dst_ref=tile(my_col, me), send_sem=bxs_sem.at[d],
                                            recv_sem=bx_sem.at[d], device_id={'row': to}, device_id_type=MESH)

    def line(d):
        return row_at(n_row - 2 * d)

    def to_col(e, d):
        t = tile(my_col, line(d))
        return pltpu.make_async_remote_copy(src_ref=t, dst_ref=t, send_sem=bys_sem.at[e, d], recv_sem=by_sem.at[e, d],
                                            device_id={'col': col_at(e)}, device_id_type=MESH)

    def relay(d):
        e = 1 if d < n_chip // 2 else n_col - 1
        t = tile(col_at(n_col - e), line(d))
        return pltpu.make_async_remote_copy(src_ref=t, dst_ref=t, send_sem=bys_sem.at[2, d], recv_sem=by_sem.at[2, d],
                                            device_id={'col': col_at(e)}, device_id_type=MESH)

    def to_mate(e, d):
        t = tile(col_at(n_col - e), line(d))
        return pltpu.make_async_remote_copy(src_ref=t, dst_ref=t, send_sem=bds_sem.at[e, d], recv_sem=bd_sem.at[e, d],
                                            device_id={'row': mate}, device_id_type=MESH)

    near = (1, n_col - 1)

    def forward(d):
        for e in near:
            to_col(e, d).start()
        to_mate(0, d).start()

    for d in range(1, n_chip):
        to_chip(d).start()
    forward(0)

    def widen(col):
        def rows_of(r, _, c):
            at = pl.ds(pl.multiple_of(r * block, block), block)
            first = c * cols // LANES
            for h in range(heads):
                if c % 2 == 0:
                    bias_scr[h, first, at] = brecv[c, r, h]
                    b = brecv[c, r, heads + h // 2]
                    if h % 2:
                        b = swap_half(b.astype(F32)).astype(BF16)
                    bias_scr[h, first + 1, at, 0:HALF] = b[:, 0:HALF]
                else:
                    a = swap_half(brecv[c, r, h].astype(F32))
                    b = brecv[c, r, heads + h // 2].astype(F32)
                    b = b if h % 2 else swap_half(b)
                    bias_scr[h, first, at, HALF:LANES] = a.astype(BF16)[:, HALF:LANES]
                    bias_scr[h, first + 1, at] = jnp.where(low, a, b).astype(BF16)
            return 0

        for c in range(n_col):
            @pl.when(col == c)
            def _():
                lax.fori_loop(0, n_row, functools.partial(rows_of, c=c), 0)

    def arrived(c):
        pltpu.make_async_copy(zin.at[c], zin.at[c], zin_sem.at[c]).wait()

    def prepare(c):
        norm_group(zin, c, gamma, beta, a_scr)
        project_group(rows, a_scr, w_kk, w_qvg_t, fill_scr, k_scr, q_scr, v_scr, g_scr, head_dim)

    for d in sorted(range(1, n_chip), key=lambda d: min(d, n_chip - d)):
        to_chip(d).wait_recv()
        forward(d)
    send_group(0, early, block - early)
    for d in range(n_chip):
        to_mate(0, d).wait_recv()
    widen(my_col)
    arrived(0)
    send_group(1)
    norm_group(zin, 0, gamma, beta, a_scr)
    for d in range(n_chip):
        for e in near:
            to_col(e, d).wait_recv()
            to_mate(e, d).start()
        relay(d).start()
    project_group(rows, a_scr, w_kk, w_qvg_t, fill_scr, k_scr, q_scr, v_scr, g_scr, head_dim)
    for e in near:
        for d in range(n_chip):
            to_mate(e, d).wait_recv()

    def widen_near(t, _):
        widen(lax.rem(my_col + 1 + t * (n_col - 2), n_col))
        return 0

    lax.fori_loop(0, 2, widen_near, 0)

    def far_to_mate():
        for d in range(n_chip):
            relay(d).wait_recv()
            to_mate(2, d).start()

    def far_ready():
        for d in range(n_chip):
            to_mate(2, d).wait_recv()
        widen(col_at(2))

    n_block = rows // LANES
    n_pair = GROUP // 2
    per_block = n_pair // UNROLL

    def group(c, _):
        first = (my_col + 1) // 2
        chip = me // 2
        last = chip + (chip + 1) // 2

        def block_at(b):
            paired = lax.rem(b // 2 + first, n_block // 2) * 2 + lax.rem(b, 2)
            return jnp.where(c == 0, paired, lax.rem(b + last + 1, n_block))

        def where(u):
            return lax.rem(u, n_pair), block_at(u // n_pair)

        for h in range(heads):
            pair, ib = where(0)
            scores(pair, ib, h, rows, tail_scr, bias_scr, k_scr, q_scr, s_scr, top_scr)

        def one_block(b, _):
            def one(u, _):
                @pl.when((c == 0) & (u == (GROUP // 2 - 2) // UNROLL))
                def _():
                    far_to_mate()

                @pl.when((c == 0) & (u == (GROUP - 2) // UNROLL))
                def _():
                    far_ready()

                for v in range(UNROLL):
                    pair, ib = where(u * UNROLL + v)
                    npair, nib = where(jnp.minimum(u * UNROLL + v + 1, n_pair * n_block - 1))
                    for h in range(heads):
                        soft_and_next(pair, ib, npair, nib, h, rows, tail_scr, bias_scr, k_scr, q_scr, v_scr, g_scr, s_scr, top_scr, o_scr)
                return 0

            lax.fori_loop(b * per_block, (b + 1) * per_block, one, 0)
            lo = pl.multiple_of(block_at(b) * LANES, LANES)

            for j in range(GROUP):
                gated = o_scr[j, :, :, pl.ds(lo, LANES)].reshape(heads * head_dim, LANES)
                a_scr[pl.ds(lo * GROUP + j, LANES, stride=GROUP), :] = lax.dot_general(gated, w_o[...], TN, preferred_element_type=F32)

            def finish(t, _):
                at = pl.multiple_of(lo + t * HALF, HALF)
                upd = a_scr[pl.ds(pl.multiple_of(at * GROUP, HALF * GROUP), HALF * GROUP), :].reshape(HALF, GROUP, chan)
                zin[c, pl.ds(at, HALF)] = (zin[c, pl.ds(at, HALF)].astype(F32) + upd).astype(BF16)
                return 0

            lax.fori_loop(0, LANES // HALF, finish, 0)

            def send(t, _):
                seg = lo // PIECE + t
                to = seg // (block // PIECE)
                off = lax.rem(seg, block // PIECE) * PIECE
                src = zin.at[c, pl.ds(pl.multiple_of(seg * PIECE, PIECE), PIECE)]
                dst = out_ref.at[pl.ds(pl.multiple_of(off, PIECE), PIECE), pl.ds(pl.multiple_of(me * share + c * GROUP, GROUP), GROUP), :]

                @pl.when(to == me)
                def _():
                    pltpu.make_async_copy(src, dst, out_sem).start()

                @pl.when(to != me)
                def _():
                    pltpu.make_async_remote_copy(src_ref=src, dst_ref=dst, send_sem=osend_sem, recv_sem=out_sem,
                                                 device_id={'row': to}, device_id_type=MESH).start()
                return 0

            lax.fori_loop(0, LANES // PIECE, send, 0)
            return 0

        lax.fori_loop(0, n_block, one_block, 0)

        @pl.when(c < n_group - 1)
        def _():
            arrived(c + 1)

            @pl.when(c < n_group - 2)
            def _():
                send_group(c + 2)

            prepare(c + 1)
        return 0

    lax.fori_loop(0, n_group, group, 0)

    for s in range(1, n_row):
        pltpu.make_async_copy(z_ref.at[:, 0:share, :], z_ref.at[:, 0:share, :], zsend_sem.at[s]).wait()
    for d in range(1, n_chip):
        to_chip(d).wait_send()
    for d in range(n_chip):
        for e in near:
            to_col(e, d).wait_send()
        relay(d).wait_send()
        for e in range(n_col):
            to_mate(e, d).wait_send()
    pltpu.make_async_copy(zin.at[:, 0:rows - block], zin.at[:, 0:rows - block], osend_sem).wait()
    pltpu.make_async_copy(z_ref, out_ref, out_sem).wait()


def run(n_row, n_col, z, mask, gamma, beta, w_q, w_k, w_v, w_b, w_g, w_o):
    block, cols, chan = z.shape
    rows, share, proj = block * n_row, cols // n_row, w_k.shape[1]
    heads = w_b.shape[0]
    n_group, n_chip, head_dim = share // GROUP, n_row // 2, proj // heads
    vmem = pl.BlockSpec(memory_space=pltpu.VMEM)
    hbm = pl.BlockSpec(memory_space=pl.ANY)
    dma = pltpu.SemaphoreType.DMA
    return pl.pallas_call(
        functools.partial(kernel, n_row, n_col, heads),
        out_shape=jax.ShapeDtypeStruct(z.shape, BF16),
        in_specs=[hbm] + [vmem] * 9,
        out_specs=hbm,
        scratch_shapes=[
            pltpu.VMEM((3 * proj, chan), BF16),
            pltpu.VMEM((8, chan), BF16),
            pltpu.VMEM((2 * chan, heads * LANES), BF16),
            pltpu.VMEM((2 * LANES - 2 * head_dim, 2 * LANES), BF16),
            pltpu.VMEM((rows, LANES), BF16),
            pltpu.VMEM((block, cols, chan), BF16),
            pltpu.VMEM((n_group, rows, GROUP, chan), BF16),
            pltpu.VMEM((n_col, n_row, heads + heads // 2, block, LANES), BF16),
            pltpu.VMEM((2 * 8 * block, LANES), F32),
            pltpu.VMEM((rows * GROUP, chan), F32),
            pltpu.VMEM((GROUP // 2, heads, rows, LANES), BF16),
            pltpu.VMEM((GROUP // 2, heads, rows // LANES, 2 * head_dim, 2 * LANES), BF16),
            pltpu.VMEM((GROUP // 2, heads, 2 * head_dim, rows), BF16),
            pltpu.VMEM((GROUP, heads, head_dim, rows), F32),
            pltpu.VMEM((heads, rows // LANES, rows, LANES), BF16),
            pltpu.VMEM((heads, rows, BLOCK), F32),
            pltpu.VMEM((heads, 1, BLOCK), F32),
            pltpu.VMEM((GROUP, heads, head_dim, rows), BF16),
            dma((4,)), dma((n_group,)), dma((n_row,)), dma((n_chip,)), dma((n_chip,)), dma((n_col, n_chip)), dma((n_col, n_chip)),
            dma((n_col, n_chip)), dma((n_col, n_chip)), dma, dma,
        ],
        compiler_params=pltpu.CompilerParams(vmem_limit_bytes=62 * 1024 * 1024, collective_id=0, has_side_effects=True),
        name="triangle",
    )(z, mask, gamma, beta, w_q, w_k, w_v, w_b, w_g, w_o)


def copy_out(x, pieces=8):
    step = x.shape[0] // pieces

    def body(x_ref, o_ref, buf, in_sem, out_sem):
        def part(n):
            return pl.ds(n * step, step)

        loads = [pltpu.make_async_copy(x_ref.at[part(n)], buf.at[part(n)], in_sem.at[n]) for n in range(pieces)]
        stores = [pltpu.make_async_copy(buf.at[part(n)], o_ref.at[part(n)], out_sem.at[n]) for n in range(pieces)]
        for load in loads:
            load.start()
        for load, store in zip(loads, stores):
            load.wait()
            store.start()
        for store in stores:
            store.wait()

    hbm = pl.BlockSpec(memory_space=pltpu.HBM)
    return pl.pallas_call(
        body,
        out_shape=jax.ShapeDtypeStruct(x.shape, x.dtype),
        in_specs=[hbm],
        out_specs=hbm,
        scratch_shapes=[pltpu.VMEM(x.shape, x.dtype), pltpu.SemaphoreType.DMA((pieces,)), pltpu.SemaphoreType.DMA((pieces,))],
        compiler_params=pltpu.CompilerParams(vmem_limit_bytes=62 * 1024 * 1024),
        name="copy_out",
    )(x)


def solution(mesh):
    n_row, n_col = mesh.shape['row'], mesh.shape['col']

    def body(pair_tile, res_mask, ln_gamma, ln_beta, w_q, w_k, w_v, w_b, w_g, w_o):
        out = run(n_row, n_col, pair_tile, res_mask.reshape(-1, LANES), ln_gamma[None], ln_beta[None], w_q, w_k, w_v, w_b.T, w_g, w_o)
        return copy_out(out)

    tile_spec = P(('data', 'row'), 'col', None)
    return jax.shard_map(body, mesh=mesh, in_specs=(tile_spec, P('data'), P(), P(), P(), P(), P(), P(), P(), P()), out_specs=tile_spec, check_vma=False)
```
